256 devices in a mesh: batch: 16 (over y, x), field: 2 (over core), dim: 8 (over z).
Axes of the slice: x: 4, y: 4, z: 8, core: 2. Of those that a mesh axis runs over, the one named last changes fastest.
Arguments:
- features: bfloat16 [26, 128, 16384], P('field', 'dim', 'batch'), may hold values from -6 to 6
- cross_weight: bfloat16 [2, 26, 128, 26, 128], P(None, 'field', 'dim'), may hold values from -0.109375 to 0.109375
- cross_bias: float32 [2, 26, 128], P(None, 'field', 'dim'), may hold values from -3 to 3
- tower_weight: bfloat16 [1024, 26, 128], P(('field', 'dim')), may hold values from -0.109375 to 0.109375
- tower_bias: float32 [1024], P(('field', 'dim')), may hold values from -3 to 3
- query_weight: bfloat16 [1024, 128], P(('field', 'dim')), may hold values from -0.1875 to 0.1875
- user_vec: bfloat16 [16384, 128], P('batch'), may hold values from -6 to 6
- candidates: bfloat16 [4096, 128], P('batch'), may hold values from -6 to 6
- positive: int32 [16384], P('batch'), may hold values from 0 to 4095
Outputs:
- crossed: bfloat16 [26, 128, 16384], P('field', 'dim', 'batch')
- losses: float32 [16384], P('batch')
The draws below stay inside these ranges and needn't reach their ends.
All inputs are finite; a program needn't handle non-finite values.
Results may differ from the reference program's by a relative error of at most 0.0049.
Values may be sent and summed in bfloat16 or wider, within the bound.
No kernel may reach another device: no remote copies, remote signals or barrier semaphores. Data moves between devices by JAX's collectives and lax.ppermute only.
A program may use at most 64 MiB of HBM per device.

```python
import math
import jax
import jax.numpy as jnp
from jax import lax

FIELDS = 26
EMB = 128
TOWER = 1024
CROSS = 2
EX_DEV = 1024
BATCH = 16384
CANDS = 4096
N_BATCH = 16


def draw_user_vec(key, part):
    row_total = BATCH
    values = jnp.clip(jax.random.normal(jax.random.fold_in(key, 11), (row_total, EMB), jnp.float32), -6.0, 6.0)
    return values.astype(jnp.bfloat16)


def draw_candidates(key, part):
    row_total = CANDS
    values = jnp.clip(jax.random.normal(jax.random.fold_in(key, 23), (row_total, EMB), jnp.float32), -6.0, 6.0)
    return values.astype(jnp.bfloat16)


def plant(entries, rng, low, top_value):
    extent = entries.shape
    spot = [jax.random.randint(jax.random.fold_in(rng, axis), (), 0, extent[axis]) for axis in range(len(extent))]
    entries = entries.at[tuple(spot)].set(low)
    longest = extent.index(max(extent))
    spot[longest] = (spot[longest] + 1) % extent[longest]
    return entries.at[tuple(spot)].set(top_value)


def steps_of(rng, dims, split, least, largest):
    loudness = 1.0
    for dim, parts in split:
        draws = jax.random.uniform(jax.random.fold_in(jax.random.fold_in(rng, 6), dim), (parts,), jnp.float32, least / len(split), largest / len(split))
        loudness = loudness * jnp.repeat(jnp.exp(draws), dims[dim] // parts).reshape((-1,) + (1,) * (len(dims) - 1 - dim))
    return loudness


def normal_values(own_key, shape, deviation, most, cuts=(), kind=jnp.bfloat16):
    values = deviation * jax.random.normal(own_key, shape, jnp.float32)
    if cuts:
        values = values * steps_of(own_key, shape, cuts, -0.22, 0.18)
    return jnp.clip(values, -most, most).astype(kind)


def setup_inputs(seed: int = 0) -> dict:
    key_of = jax.random.split(jax.random.key(seed), 10)
    return {
        "features": normal_values(key_of[0], (FIELDS, EMB, BATCH), 1.0, 6.0, ((0, 2), (1, 8), (2, 16))),
        "cross_weight": normal_values(key_of[1], (CROSS, FIELDS, EMB, FIELDS, EMB), (FIELDS * EMB) ** -0.5, 0.109375, ((1, 2), (2, 8))),
        "cross_bias": normal_values(key_of[2], (CROSS, FIELDS, EMB), 0.5, 3.0, ((1, 2), (2, 8)), jnp.float32),
        "tower_weight": normal_values(key_of[3], (TOWER, FIELDS, EMB), (FIELDS * EMB) ** -0.5, 0.109375, ((0, 16),)),
        "tower_bias": normal_values(key_of[4], (TOWER,), 0.5, 3.0, ((0, 16),), jnp.float32),
        "query_weight": normal_values(key_of[5], (TOWER, EMB), TOWER ** -0.5, 0.1875, ((0, 16),)),
        "user_vec": draw_user_vec(jax.random.fold_in(key_of[9], 71), 0),
        "candidates": draw_candidates(jax.random.fold_in(key_of[9], 71), 0),
        "positive": plant(jax.random.randint(key_of[8], (BATCH,), 0, CANDS), jax.random.fold_in(key_of[8], 1), 0, CANDS - 1).astype(jnp.int32),
    }


def reference(features, cross_weight, cross_bias, tower_weight, tower_bias, query_weight, user_vec, candidates, positive):
    width_all = FIELDS * EMB
    anchor = features.reshape(width_all, BATCH).T
    current = anchor
    for level_idx in range(CROSS):
        matrix = cross_weight[level_idx].reshape(width_all, width_all).T
        product = jnp.dot(current, matrix, preferred_element_type=jnp.float32) + cross_bias[level_idx].reshape(width_all)
        current = (anchor.astype(jnp.float32) * product + current.astype(jnp.float32)).astype(jnp.bfloat16)
    crossed = current.T.reshape(FIELDS, EMB, BATCH)
    tower_matrix = tower_weight.reshape(TOWER, width_all).T
    hidden = jax.nn.relu(jnp.dot(current, tower_matrix, preferred_element_type=jnp.float32) + tower_bias).astype(jnp.bfloat16)
    query_vec = (jnp.dot(hidden, query_weight, preferred_element_type=jnp.float32) + user_vec.astype(jnp.float32)).astype(jnp.bfloat16)
    score_scale = 1.0 / math.sqrt(EMB)

    def block_loss(inputs):
        queries, targets = inputs
        logits = jnp.dot(queries, candidates.T, preferred_element_type=jnp.float32) * score_scale
        picked = jnp.take_along_axis(logits, targets[:, None], axis=1)[:, 0]
        return jax.nn.logsumexp(logits, axis=1) - picked
    losses = lax.map(block_loss, (query_vec.reshape(N_BATCH, EX_DEV, EMB), positive.reshape(N_BATCH, EX_DEV)))
    return (crossed, losses.reshape(BATCH))
```

```python
import functools
import math

import jax
import jax.numpy as jnp
from jax import lax
from jax.experimental import pallas as pl
from jax.experimental.pallas import tpu as pltpu
from jax.sharding import Mesh
from jax.sharding import PartitionSpec as P

CROSS = 2
BATCH = ("batch_0", "batch_1")
CHUNKS = 2


def shift(x, axis, step):
    length = lax.axis_size(axis)
    return lax.ppermute(x, axis, [(i, (i + step) % length) for i in range(length)])


def ring_gather(block, axis, forward):
    length = lax.axis_size(axis)
    up = length // 2 if forward else length - 1 - length // 2
    down = length - 1 - up
    found = [(0, block)]
    rising = falling = block
    for step in range(1, max(up, down) + 1):
        if step <= up:
            rising = shift(rising, axis, 1)
            found.append((-step, rising))
        if step <= down:
            falling = shift(falling, axis, -1)
            found.append((step, falling))
    return found


def order_kernel(place_ref, own_ref, other_ref, out_ref):
    core = place_ref[0]
    fields = own_ref.shape[1]
    rows = own_ref.shape[0] * own_ref.shape[2]
    lanes = own_ref.shape[3]
    half = fields // 2
    for group in range(fields):
        source = lax.rem(core + group // half, 2) * half + group % half
        span = slice(group * lanes, (group + 1) * lanes)
        out_ref[:rows, span] = own_ref[:, source].reshape(rows, lanes)
        out_ref[rows:, span] = other_ref[:, source].reshape(rows, lanes)


def ordered_weight(place, own, other):
    rows = 2 * own.shape[0] * own.shape[2]
    return pl.pallas_call(
        order_kernel,
        out_shape=jax.ShapeDtypeStruct((rows, own.shape[1] * own.shape[3]), own.dtype),
        in_specs=[pl.BlockSpec(memory_space=pltpu.SMEM)] + [pl.BlockSpec(memory_space=pltpu.VMEM)] * 2,
        out_specs=pl.BlockSpec(memory_space=pltpu.VMEM),
    )(place, own, other)


def gather_in_place(place_ref, block_refs, offsets, whole_ref):
    position = place_ref[1]
    length = len(offsets)
    for offset, block_ref in zip(offsets, block_refs):
        source = lax.rem(position + offset + length, length)
        whole_ref[:, source] = block_ref[...]
    fields, planes, entries, rows = whole_ref.shape
    return whole_ref[...].reshape(fields * planes * entries, rows)


def layer_kernel(offsets, place_ref, weight_ref, bias_ref, anchor_ref, *refs):
    blocks, out_ref, whole_ref = refs[: len(offsets)], refs[-2], refs[-1]
    inputs = gather_in_place(place_ref, blocks, offsets, whole_ref)
    shape = anchor_ref.shape
    product = jnp.dot(weight_ref[...], inputs, preferred_element_type=jnp.float32)
    gated = product + bias_ref[:, :1]
    flat = (shape[0] * shape[1], shape[2])
    anchor = anchor_ref[...].reshape(flat).astype(jnp.float32)
    current = blocks[0][...].reshape(flat).astype(jnp.float32)
    out_ref[...] = (anchor * gated + current).astype(jnp.bfloat16).reshape(shape)


def tower_kernel(offsets, place_ref, weight_ref, bias_ref, query_ref, *refs):
    blocks, out_ref, whole_ref = refs[: len(offsets)], refs[-2], refs[-1]
    inputs = gather_in_place(place_ref, blocks, offsets, whole_ref)
    product = jnp.dot(weight_ref[...], inputs, preferred_element_type=jnp.float32)
    hidden = jax.nn.relu(product + bias_ref[:, :1]).astype(jnp.bfloat16)
    partial = lax.dot_general(
        hidden, query_ref[...], (((0,), (0,)), ((), ())), preferred_element_type=jnp.float32
    )
    out_ref[...] = partial.astype(jnp.bfloat16)


def on_blocks(kernel, place, leading, found, out_shape):
    offsets = tuple(offset for offset, _ in found)
    blocks = [block for _, block in found]
    fields, entries, rows = blocks[0].shape
    vmem = pl.BlockSpec(memory_space=pltpu.VMEM)
    return pl.pallas_call(
        functools.partial(kernel, offsets),
        out_shape=out_shape,
        in_specs=[pl.BlockSpec(memory_space=pltpu.SMEM)] + [vmem] * (len(leading) + len(blocks)),
        out_specs=vmem,
        scratch_shapes=[pltpu.VMEM((fields, len(blocks), entries, rows), jnp.bfloat16)],
    )(place, *leading, *blocks)


def as_column(values):
    return jnp.broadcast_to(values.reshape(-1, 1), (values.size, 128))


def sent_to_all(x, axis):
    copies = jnp.broadcast_to(x, (lax.axis_size(axis), *x.shape))
    return lax.all_to_all(copies, axis, split_axis=0, concat_axis=0, tiled=True)


def whole_of(x, axes, dim):
    if not axes:
        return x
    nearer = lax.all_gather(x, axes[-1], axis=dim, tiled=True)
    return whole_of(nearer, axes[:-1], dim)


def candidate_loss(query_vec, targets, everyone):
    score_scale = 1.0 / math.sqrt(query_vec.shape[1])
    logits = (
        jnp.einsum("be,ce->bc", query_vec, everyone, preferred_element_type=jnp.float32) * score_scale
    )
    labels = lax.broadcasted_iota(jnp.int32, logits.shape, 1)
    picked = jnp.sum(jnp.where(labels == targets[:, None], logits, 0.0), axis=1)
    best = jnp.max(logits, axis=1)
    total = jnp.sum(jnp.exp(logits - best[:, None]), axis=1)
    return best + jnp.log(total) - picked


def body(
    features,
    cross_weight,
    cross_bias,
    tower_weight,
    tower_bias,
    query_weight,
    user_vec,
    candidates,
    positive,
):
    core = lax.axis_index("field")
    plane = lax.axis_index("dim")
    planes = lax.axis_size("dim")
    place = jnp.stack([core, plane]).astype(jnp.int32)
    field_local, entry_local, row_count = features.shape
    half_rows = row_count // 2
    chunk_rows = half_rows // CHUNKS

    def swap(x):
        return shift(x, "field", 1)

    mine = lax.dynamic_slice_in_dim(features, core * half_rows, half_rows, 2)
    theirs = lax.dynamic_slice_in_dim(features, (1 - core) * half_rows, half_rows, 2)
    rows_here = jnp.concatenate([mine, swap(theirs)], axis=0)
    anchors = [rows_here[:, :, i * chunk_rows : (i + 1) * chunk_rows] for i in range(CHUNKS)]

    weights = cross_weight.transpose(0, 1, 3, 2, 4)
    other_bias = swap(cross_bias)
    current = anchors
    for level in range(CROSS):
        matrix = ordered_weight(place, weights[level], swap(weights[level]))
        bias = as_column(jnp.concatenate([cross_bias[level].reshape(-1), other_bias[level].reshape(-1)]))
        current = [
            on_blocks(
                layer_kernel,
                place,
                (matrix, bias, anchors[i]),
                ring_gather(current[i], "dim", i % 2 == 0),
                jax.ShapeDtypeStruct(anchors[i].shape, jnp.bfloat16),
            )
            for i in range(CHUNKS)
        ]
    final = jnp.concatenate(current, axis=2)
    kept = final[:field_local]
    fetched = swap(final[field_local:])
    crossed = jnp.where(
        core == 0,
        jnp.concatenate([kept, fetched], axis=2),
        jnp.concatenate([fetched, kept], axis=2),
    )

    own_tower = tower_weight.transpose(1, 0, 2)[None]
    tower_matrix = ordered_weight(place, own_tower, swap(own_tower))
    tower_column = as_column(jnp.concatenate([tower_bias, swap(tower_bias)]))
    query_rows = jnp.concatenate([query_weight, swap(query_weight)], axis=0)
    partials = [
        on_blocks(
            tower_kernel,
            place,
            (tower_matrix, tower_column, query_rows),
            ring_gather(current[i], "dim", i % 2 == 0),
            jax.ShapeDtypeStruct((chunk_rows, query_weight.shape[1]), jnp.bfloat16),
        )
        for i in range(CHUNKS)
    ]
    partial = jnp.concatenate(partials, axis=0)
    share = half_rows // planes
    pieces = lax.all_to_all(
        partial.reshape(planes, share, partial.shape[1]), "dim", 0, 0, tiled=True
    )
    start = core * half_rows + plane * share
    user_rows = lax.dynamic_slice_in_dim(user_vec, start, share, 0)
    targets = lax.dynamic_slice_in_dim(positive, start, share, 0)
    query_part = jnp.sum(pieces.astype(jnp.float32), axis=0)
    query_vec = (query_part + user_rows.astype(jnp.float32)).astype(jnp.bfloat16)
    part_loss = candidate_loss(query_vec, targets, whole_of(candidates, BATCH, 0))
    losses = sent_to_all(part_loss, ("field", "dim")).reshape(row_count)
    return (crossed, losses)


def solution(mesh):
    torus = Mesh(
        mesh.devices.reshape(4, 4, mesh.shape["field"], mesh.shape["dim"]),
        ("batch_0", "batch_1", "field", "dim"),
    )
    in_specs = (
        P("field", "dim", BATCH),
        P(None, "field", "dim", None, None),
        P(None, "field", "dim"),
        P(("field", "dim"), None, None),
        P(("field", "dim")),
        P(("field", "dim"), None),
        P(BATCH, None),
        P(BATCH, None),
        P(BATCH),
    )
    out_specs = (P("field", "dim", BATCH), P(BATCH))
    return jax.shard_map(body, mesh=torus, in_specs=in_specs, out_specs=out_specs, check_vma=False)
```

```python
import functools
import math

import jax
import jax.numpy as jnp
from jax import lax
from jax.experimental import pallas as pl
from jax.experimental.pallas import tpu as pltpu
from jax.sharding import Mesh
from jax.sharding import PartitionSpec as P

CROSS = 2
BATCH = ("batch_0", "batch_1")
CHUNKS = 2
LANES = 128
WIDE = 256
SMEM = pl.BlockSpec(memory_space=pltpu.SMEM)
VMEM = pl.BlockSpec(memory_space=pltpu.VMEM)


def grant(mib):
    return pltpu.CompilerParams(vmem_limit_bytes=mib * 1024 * 1024)


def shift(x, axis, step):
    length = lax.axis_size(axis)
    return lax.ppermute(x, axis, [(i, (i + step) % length) for i in range(length)])


def ring_gather(block, axis, forward):
    length = lax.axis_size(axis)
    up = length // 2 if forward else length - 1 - length // 2
    down = length - 1 - up
    found = [(0, block)]
    rising = falling = block
    for step in range(1, max(up, down) + 1):
        if step <= up:
            rising = shift(rising, axis, 1)
            found.append((-step, rising))
        if step <= down:
            falling = shift(falling, axis, -1)
            found.append((step, falling))
    return found


def crosswise(x, step, far):
    outer, inner = (lax.axis_size(axis) for axis in BATCH)
    pairs = []
    for a in range(outer):
        for b in range(inner):
            for core in range(2):
                if (core == 0) != far:
                    target = ((a + step) % outer, b)
                else:
                    target = (a, (b + step) % inner)
                pairs.append((2 * (a * inner + b) + core, 2 * (target[0] * inner + target[1]) + core))
    return lax.ppermute(x, BATCH + ("field",), pairs)


def order_kernel(place_ref, own_ref, other_ref, out_ref):
    core = place_ref[0]
    fields = own_ref.shape[1]
    rows = own_ref.shape[0] * own_ref.shape[2]
    lanes = own_ref.shape[3]
    half = fields // 2

    def step(k, _):
        for part in range(2):
            group = 2 * k + part
            high = (group >= half).astype(jnp.int32)
            source = lax.rem(core + high, 2) * half + group - high * half
            span = slice(part * lanes, (part + 1) * lanes)
            out_ref[k, :rows, span] = own_ref[:, source].reshape(rows, lanes)
            out_ref[k, rows:, span] = other_ref[:, source].reshape(rows, lanes)
        return 0

    lax.fori_loop(0, fields // 2, step, 0)


def ordered_weight(place, own, other):
    rows = 2 * own.shape[0] * own.shape[2]
    return pl.pallas_call(
        order_kernel,
        out_shape=jax.ShapeDtypeStruct((own.shape[1] // 2, rows, 2 * own.shape[3]), own.dtype),
        in_specs=[SMEM, VMEM, VMEM],
        out_specs=VMEM,
        compiler_params=grant(12),
    )(place, own, other)


def layer_kernel(offsets, last, place_ref, weight_ref, bias_ref, anchor_ref, *refs):
    blocks = refs[: len(offsets)]
    outs, (whole_ref, sum_ref) = refs[len(offsets) : -2], refs[-2:]
    plane = place_ref[1]
    length = len(offsets)
    for offset, block_ref in zip(offsets, blocks):
        whole_ref[:, lax.rem(plane + offset + length, length)] = block_ref[...]
    shape = anchor_ref.shape
    rows = shape[2]
    sum_ref[...] = jnp.broadcast_to(bias_ref[:, :1], sum_ref.shape)

    def step(k, _):
        part = whole_ref[pl.ds(2 * k, 2)].reshape(2 * LANES, rows)
        sum_ref[...] += jnp.dot(weight_ref[k], part, preferred_element_type=jnp.float32)
        return 0

    lax.fori_loop(0, weight_ref.shape[0], step, 0)
    flat = (shape[0] * shape[1], rows)
    anchor = anchor_ref[...].reshape(flat).astype(jnp.float32)
    current = blocks[0][...].reshape(flat).astype(jnp.float32)
    result = (anchor * sum_ref[...] + current).astype(jnp.bfloat16)
    outs[0][...] = result.reshape(shape)
    if last:
        halves = result.reshape(2, flat[0] // 2, rows).astype(jnp.float32)
        spare = WIDE - flat[0] // 2
        line = lax.broadcasted_iota(jnp.int32, (spare, rows), 0)
        ones = jnp.where((line >= 16) & (line < 19), 1.0, 0.0)
        turned = [
            jnp.concatenate([halves[h], ones], axis=0).T.astype(jnp.bfloat16) for h in range(2)
        ]
        share = rows // length
        turn_ref = outs[-1]
        for h in range(2):
            turn_ref[:, :, h * WIDE : (h + 1) * WIDE] = turned[h].reshape(length, share, WIDE)
        for k in range(length):
            outs[1 + k][...] = turn_ref[lax.rem(plane + k, length)]


def cross_layer(place, matrix, bias, anchor, found, last):
    offsets = tuple(offset for offset, _ in found)
    blocks = [block for _, block in found]
    fields, entries, rows = anchor.shape
    planes = len(blocks)
    share = rows // planes
    out_shape = [jax.ShapeDtypeStruct(anchor.shape, jnp.bfloat16)]
    if last:
        out_shape += [jax.ShapeDtypeStruct((share, 2 * WIDE), jnp.bfloat16)] * planes
    scratch = [
        pltpu.VMEM((fields, planes, entries, rows), jnp.bfloat16),
        pltpu.VMEM((fields * entries, rows), jnp.float32),
    ]
    if last:
        scratch = [pltpu.VMEM((planes, share, 2 * WIDE), jnp.bfloat16)] + scratch
    return pl.pallas_call(
        functools.partial(layer_kernel, offsets, last),
        out_shape=out_shape,
        in_specs=[SMEM] + [VMEM] * (3 + planes),
        out_specs=[VMEM] * len(out_shape),
        scratch_shapes=scratch,
        compiler_params=grant(14),
    )(place, matrix, bias, anchor, *blocks)


def pick_kernel(place_ref, tower_ref, bias_ref, query_ref, candidate_ref, piece_ref, line_ref):
    core, high, group = place_ref[0], place_ref[2], place_ref[3]
    count = piece_ref.shape[0]
    half = tower_ref.shape[0] // 2
    entries = 16
    planes = LANES // entries
    start = pl.multiple_of(group * count, count)
    lane = lax.broadcasted_iota(jnp.int32, (count, LANES), 1)
    sources = [
        tower_ref[high * half + f, pl.ds(start, count)].astype(jnp.float32) for f in range(half)
    ]
    query = query_ref[pl.ds(start, count)].astype(jnp.float32)
    bias = bias_ref[pl.ds(start, count)]
    first = bias.astype(jnp.bfloat16).astype(jnp.float32)
    second = (bias - first).astype(jnp.bfloat16).astype(jnp.float32)
    third = bias - first - second
    bias_lanes = jnp.where(
        lane == 96, first, jnp.where(lane == 97, second, jnp.where(lane == 98, third, 0.0))
    )
    bias_lanes = jnp.where(high == 0, bias_lanes, 0.0)
    for plane in range(planes):
        for tile in range(2):
            kept = bias_lanes if (tile == 1 and plane == 0) else jnp.zeros((count, LANES), jnp.float32)
            inside = [(f % 8, sources[f]) for f in range(half) if f // 8 == tile]
            if tile == 1:
                inside.append((5, query))
            for slot, source in inside:
                moved = pltpu.roll(source, ((slot - plane) * entries) % LANES, 1)
                kept = jnp.where((lane >= slot * entries) & (lane < (slot + 1) * entries), moved, kept)
            at = plane * WIDE + tile * LANES
            piece_ref[:, at : at + LANES] = kept.astype(jnp.bfloat16)
    lines = line_ref.shape[1] // LANES
    for t in range(lines):
        at = pl.multiple_of(core * lines * count + t * count, count)
        line_ref[:, t * LANES : (t + 1) * LANES] = candidate_ref[pl.ds(at, count)]


def loss_kernel(offsets, near, scale, place_ref, user_ref, target_ref, *refs):
    planes = len(offsets)
    pieces, arrays = refs[:planes], refs[planes : planes + 8]
    out_ref, input_ref, score_ref = refs[planes + 8 :]
    core, plane, home = place_ref[0], place_ref[1], (place_ref[4], place_ref[5])
    rows = user_ref.shape[0]
    for offset, piece_ref in zip(offsets, pieces):
        source = lax.rem(plane + offset + planes, planes)
        for h in range(2):
            input_ref[h, source] = piece_ref[:, h * WIDE : (h + 1) * WIDE]

    def inputs(which):
        at = lax.rem(which + core, 2)
        return jnp.concatenate([input_ref[at, z] for z in range(planes)], axis=1)

    small, block, width = arrays[0].shape
    units = block - 8
    gathered = jnp.zeros((rows, planes * LANES), jnp.float32)
    for owner in range(2):
        from_core = lax.rem(core + owner, 2)
        spot = jnp.where(from_core == 0, home[1], home[0])
        for first, second, step in ((0, 3, 0), (1, 2, 1)):
            which = lax.rem(spot + step, 4) // 2
            a_ref, b_ref = arrays[4 * owner + first], arrays[4 * owner + second]
            a = a_ref[:, :units].reshape(small * units, width)
            b = b_ref[:, :units].reshape(small * units, width)
            contract = (((1,), (1,)), ((), ()))
            pre = lax.dot_general(inputs(which), a, contract, preferred_element_type=jnp.float32)
            pre += lax.dot_general(inputs(1 - which), b, contract, preferred_element_type=jnp.float32)
            hidden = jnp.maximum(pre, 0.0).astype(jnp.bfloat16)
            tails = jnp.concatenate(
                [a[:, z * WIDE + LANES : (z + 1) * WIDE] for z in range(planes)], axis=1
            )
            gathered += jnp.dot(hidden, tails, preferred_element_type=jnp.float32)
    lane = lax.broadcasted_iota(jnp.int32, (rows, LANES), 1)
    query = user_ref[...].astype(jnp.float32)
    part = jnp.zeros((rows, LANES), jnp.float32)
    for z in range(planes):
        moved = pltpu.roll(gathered[:, z * LANES : (z + 1) * LANES], ((z - 5) * 16) % LANES, 1)
        part = jnp.where((lane >= z * 16) & (lane < (z + 1) * 16), moved, part)
    query = (part + query).astype(jnp.bfloat16)
    picked = jnp.zeros((rows, 1), jnp.float32)
    best = jnp.full((rows, 1), -1e30, jnp.float32)
    lines = width // LANES
    count = lines * 8
    target = target_ref[:, :1]
    wide_lane = lax.broadcasted_iota(jnp.int32, (rows, count), 1)
    for owner in range(2):
        from_core = lax.rem(core + owner, 2)
        for number, far_offset in enumerate((0, 1, 3, 2)):
            for slot, near_offset in enumerate(near):
                block_ref = arrays[4 * owner + number]
                rows_of = jnp.concatenate(
                    [block_ref[slot, units:, t * LANES : (t + 1) * LANES] for t in range(lines)], axis=0
                )
                logits = (
                    lax.dot_general(
                        query, rows_of, (((1,), (1,)), ((), ())), preferred_element_type=jnp.float32
                    )
                    * scale
                )
                outer = lax.rem(home[0] + jnp.where(from_core == 0, near_offset, far_offset), 4)
                inner = lax.rem(home[1] + jnp.where(from_core == 0, far_offset, near_offset), 4)
                base = (outer * 4 + inner) * (2 * count) + from_core * count
                picked += jnp.sum(
                    jnp.where(wide_lane == target - base, logits, 0.0), axis=1, keepdims=True
                )
                best = jnp.maximum(best, jnp.max(logits, axis=1, keepdims=True))
                score_ref[(4 * owner + number) * 4 + slot] = logits
    total = jnp.zeros((rows, 1), jnp.float32)
    for i in range(score_ref.shape[0]):
        total += jnp.sum(jnp.exp(score_ref[i] - best), axis=1, keepdims=True)
    loss = best + jnp.log(total) - picked
    row = lax.broadcasted_iota(jnp.int32, (rows, LANES), 0)
    out_ref[...] = jnp.sum(jnp.where(lane == row, loss, 0.0), axis=0, keepdims=True)


def as_column(values):
    return jnp.broadcast_to(values.reshape(-1, 1), (values.size, LANES))


def sent_to_all(x, axis):
    copies = jnp.broadcast_to(x, (lax.axis_size(axis), *x.shape))
    return lax.all_to_all(copies, axis, split_axis=0, concat_axis=0, tiled=True)


def body(
    features,
    cross_weight,
    cross_bias,
    tower_weight,
    tower_bias,
    query_weight,
    user_vec,
    candidates,
    positive,
):
    core = lax.axis_index("field")
    plane = lax.axis_index("dim")
    planes = lax.axis_size("dim")
    home = [lax.axis_index(axis) for axis in BATCH]
    field_local, entry_local, row_count = features.shape
    half_rows = row_count // 2
    chunk_rows = half_rows // CHUNKS
    share = chunk_rows // planes
    near_spot = jnp.where(core == 0, home[0], home[1])
    far_spot = jnp.where(core == 0, home[1], home[0])
    place = jnp.stack(
        [core, plane, far_spot // 2, 2 * near_spot + far_spot % 2, home[0], home[1]]
    ).astype(jnp.int32)

    def swap(x):
        return shift(x, "field", 1)

    mine = lax.dynamic_slice_in_dim(features, core * half_rows, half_rows, 2)
    theirs = lax.dynamic_slice_in_dim(features, (1 - core) * half_rows, half_rows, 2)
    rows_here = jnp.concatenate([mine, swap(theirs)], axis=0)
    anchors = [rows_here[:, :, i * chunk_rows : (i + 1) * chunk_rows] for i in range(CHUNKS)]

    units = tower_weight.shape[0]
    width = planes * WIDE
    piece, line = pl.pallas_call(
        pick_kernel,
        out_shape=[jax.ShapeDtypeStruct((8, width), jnp.bfloat16)] * 2,
        in_specs=[SMEM] + [VMEM] * 4,
        out_specs=[VMEM] * 2,
        compiler_params=grant(4),
    )(place, tower_weight.transpose(1, 0, 2), as_column(tower_bias), query_weight, candidates)
    stack = jnp.concatenate([p for _, p in ring_gather(piece, "dim", True)] + [line], axis=0)
    near_up = crosswise(stack, 1, False)
    near_down = crosswise(stack, -1, False)
    near_two = crosswise(stack, 2, False)
    near = (0, 3, 1, 2)
    block = jnp.stack([stack, near_up, near_down, near_two])
    far_down = crosswise(block, -1, True)
    far_up = crosswise(block, 1, True)
    far_two = crosswise(far_up, 1, True)
    own_arrays = [block, far_down, far_up, far_two]
    arrays = own_arrays + [swap(a) for a in own_arrays]

    weights = cross_weight.transpose(0, 1, 3, 2, 4)
    other_bias = swap(cross_bias)
    current = anchors
    for level in range(CROSS):
        matrix = ordered_weight(place, weights[level], swap(weights[level]))
        bias = as_column(jnp.concatenate([cross_bias[level].reshape(-1), other_bias[level].reshape(-1)]))
        results = [
            cross_layer(
                place,
                matrix,
                bias,
                anchors[i],
                ring_gather(current[i], "dim", i % 2 == 0),
                level == CROSS - 1,
            )
            for i in range(CHUNKS)
        ]
        current = [result[0] for result in results]

    final = jnp.concatenate(current, axis=2)
    kept = final[:field_local]
    fetched = swap(final[field_local:])
    crossed = jnp.where(
        core == 0,
        jnp.concatenate([kept, fetched], axis=2),
        jnp.concatenate([fetched, kept], axis=2),
    )

    parts = []
    for i in range(CHUNKS):
        outgoing = results[i][1:]
        pieces = [(0, outgoing[0])] + [(-k, shift(outgoing[k], "dim", k)) for k in range(1, planes)]
        start = core * half_rows + i * chunk_rows + plane * share
        user_rows = lax.dynamic_slice_in_dim(user_vec, start, share, 0)
        targets = lax.dynamic_slice_in_dim(positive, start, share, 0)
        loss = pl.pallas_call(
            functools.partial(
                loss_kernel,
                tuple(offset for offset, _ in pieces),
                near,
                1.0 / math.sqrt(query_weight.shape[1]),
            ),
            out_shape=jax.ShapeDtypeStruct((1, LANES), jnp.float32),
            in_specs=[SMEM] + [VMEM] * (2 + planes + len(arrays)),
            out_specs=VMEM,
            scratch_shapes=[
                pltpu.VMEM((2, planes, share, WIDE), jnp.bfloat16),
                pltpu.VMEM((32, share, LANES), jnp.float32),
            ],
            compiler_params=grant(18),
        )(place, user_rows, as_column(targets), *[p for _, p in pieces], *arrays)
        parts.append(loss[0, :share])
    everyone = sent_to_all(jnp.concatenate(parts)[None], ("field", "dim"))
    losses = everyone.reshape(2, planes, CHUNKS, share).transpose(0, 2, 1, 3).reshape(row_count)
    return (crossed, losses)


def solution(mesh):
    torus = Mesh(
        mesh.devices.reshape(4, 4, mesh.shape["field"], mesh.shape["dim"]),
        ("batch_0", "batch_1", "field", "dim"),
    )
    in_specs = (
        P("field", "dim", BATCH),
        P(None, "field", "dim", None, None),
        P(None, "field", "dim"),
        P(("field", "dim"), None, None),
        P(("field", "dim")),
        P(("field", "dim"), None),
        P(BATCH, None),
        P(BATCH, None),
        P(BATCH),
    )
    out_specs = (P("field", "dim", BATCH), P(BATCH))
    return jax.shard_map(body, mesh=torus, in_specs=in_specs, out_specs=out_specs, check_vma=False)
```

```python
import functools
import math

import jax
import jax.numpy as jnp
from jax import lax
from jax.experimental import pallas as pl
from jax.experimental.pallas import tpu as pltpu
from jax.sharding import Mesh
from jax.sharding import PartitionSpec as P


CROSS = 2
BATCH = ("batch_0", "batch_1")
CHUNKS = 2
LANES = 128
WIDE = 256
SMEM = pl.BlockSpec(memory_space=pltpu.SMEM)
VMEM = pl.BlockSpec(memory_space=pltpu.VMEM)
ANY = pl.BlockSpec(memory_space=pl.ANY)


def grant(mib):
    return pltpu.CompilerParams(vmem_limit_bytes=mib * 1024 * 1024)


def shift(x, axis, step):
    length = lax.axis_size(axis)
    return lax.ppermute(x, axis, [(i, (i + step) % length) for i in range(length)])


def ring_gather(block, axis, forward):
    length = lax.axis_size(axis)
    up = length // 2 if forward else length - 1 - length // 2
    down = length - 1 - up
    found = [(0, block)]
    rising = falling = block
    for step in range(1, max(up, down) + 1):
        if step <= up:
            rising = shift(rising, axis, 1)
            found.append((-step, rising))
        if step <= down:
            falling = shift(falling, axis, -1)
            found.append((step, falling))
    return found


def crosswise(x, step, far):
    outer, inner = (lax.axis_size(axis) for axis in BATCH)
    pairs = []
    for a in range(outer):
        for b in range(inner):
            for core in range(2):
                if (core == 0) != far:
                    target = ((a + step) % outer, b)
                else:
                    target = (a, (b + step) % inner)
                pairs.append((2 * (a * inner + b) + core, 2 * (target[0] * inner + target[1]) + core))
    return lax.ppermute(x, BATCH + ("field",), pairs)


def order_kernel(level, place_ref, own_ref, other_ref, bias_ref, other_bias_ref, out_ref, column_ref):
    core = place_ref[0]
    _, outer, fields, entries, lanes = own_ref.shape
    rows = outer * entries
    half = fields // 2

    def step(k, _):
        for part in range(2):
            group = 2 * k + part
            high = (group >= half).astype(jnp.int32)
            source = lax.rem(core + high, 2) * half + group - high * half
            span = slice(part * lanes, (part + 1) * lanes)
            out_ref[k, :rows, span] = own_ref[0, :, source].reshape(rows, lanes)
            out_ref[k, rows:, span] = other_ref[0, :, source].reshape(rows, lanes)
        return 0

    lax.fori_loop(0, fields // 2, step, 0)
    line = lax.broadcasted_iota(jnp.int32, (entries, entries), 0)
    lane = lax.broadcasted_iota(jnp.int32, (entries, entries), 1)
    for side, side_ref in enumerate((bias_ref, other_bias_ref)):
        for f in range(outer):
            values = side_ref[f, level : level + 1, :]
            turned = jnp.sum(jnp.where(line == lane, values, 0.0), axis=1, keepdims=True)
            at = side * rows + f * entries
            column_ref[at : at + entries, :] = jnp.broadcast_to(turned, (entries, LANES))


def ordered_weight(level, place, own, other, bias, other_bias):
    _, outer, fields, entries, lanes = own.shape
    rows = 2 * outer * entries
    part = pl.BlockSpec((1, outer, fields, entries, lanes), lambda i: (level, 0, 0, 0, 0))
    whole = pl.BlockSpec(bias.shape, lambda i: (0, 0, 0))
    out_shape = (
        jax.ShapeDtypeStruct((fields // 2, rows, 2 * lanes), own.dtype),
        jax.ShapeDtypeStruct((rows, LANES), jnp.float32),
    )
    return pl.pallas_call(
        functools.partial(order_kernel, level),
        grid=(1,),
        out_shape=out_shape,
        in_specs=[SMEM, part, part, whole, whole],
        out_specs=(
            pl.BlockSpec(out_shape[0].shape, lambda i: (0, 0, 0)),
            pl.BlockSpec(out_shape[1].shape, lambda i: (0, 0)),
        ),
        compiler_params=grant(14),
    )(place, own, other, bias, other_bias)


def layer_kernel(offsets, turn, place_ref, weight_ref, bias_ref, anchor_ref, *refs):
    blocks = refs[: len(offsets)]
    whole_ref, refs = refs[-1], refs[len(offsets) : -1]
    earlier, outs = refs[: turn == 2], refs[turn == 2 :]
    plane = place_ref[1]
    length = len(offsets)
    fields, _, entries, rows = whole_ref.shape
    count = fields * entries
    for offset, block_ref in zip(offsets, blocks):
        source = lax.rem(plane + offset + length, length)
        whole_ref[:, source] = block_ref[:count].reshape(fields, entries, rows)
    weight = jnp.concatenate([weight_ref[k] for k in range(weight_ref.shape[0])], axis=1)
    inputs = whole_ref[...].reshape(length * count, rows)
    product = jnp.dot(weight, inputs, preferred_element_type=jnp.float32) + bias_ref[:, :1]
    anchor = anchor_ref[:count].astype(jnp.float32)
    current = blocks[0][:count].astype(jnp.float32)
    result = (anchor * product + current).astype(jnp.bfloat16)
    outs[0][...] = result
    if turn:
        halves = result.reshape(2, count // 2, rows).astype(jnp.float32)
        spare = WIDE - count // 2
        share = rows // length
        line = lax.broadcasted_iota(jnp.int32, (spare, rows), 0)
        ones = jnp.where((line >= 16) & (line < 19), 1.0, 0.0)
        at = 0
        for early_ref in earlier:
            at = early_ref.shape[1]
            outs[1][:, :at] = early_ref[...]
        for h in range(2):
            turned = jnp.concatenate([halves[h], ones], axis=0).T.astype(jnp.bfloat16)
            span = slice(h * WIDE, (h + 1) * WIDE)
            outs[1][:, at : at + share, span] = turned.reshape(length, share, WIDE)


def cross_layer(place, matrix, bias, anchor, found, turn, earlier):
    offsets = tuple(offset for offset, _ in found)
    blocks = [block for _, block in found]
    count, rows = matrix.shape[1], anchor.shape[1]
    planes = len(blocks)
    out_shape = [jax.ShapeDtypeStruct((count, rows), jnp.bfloat16)]
    if turn:
        out_shape.append(
            jax.ShapeDtypeStruct((planes, turn * (rows // planes), 2 * WIDE), jnp.bfloat16)
        )
    return pl.pallas_call(
        functools.partial(layer_kernel, offsets, turn),
        out_shape=out_shape,
        in_specs=[SMEM] + [VMEM] * (3 + planes + len(earlier)),
        out_specs=[VMEM] * len(out_shape),
        scratch_shapes=[pltpu.VMEM((count // 16, planes, 16, rows), jnp.bfloat16)],
        compiler_params=grant(14),
    )(place, matrix, bias, anchor, *blocks, *earlier)


def cut_kernel(place_ref, feature_ref, out_ref):
    fields, entries, _ = feature_ref.shape
    half = out_ref.shape[1]
    start = pl.multiple_of((1 - place_ref[0]) * half, half)
    out_ref[...] = feature_ref[:, :, pl.ds(start, half)].reshape(fields * entries, half)


def pick_kernel(
    place_ref, feature_ref, other_ref, tower_ref, bias_ref, query_ref, piece_ref, second_ref
):
    half_count, half_rows = other_ref.shape
    first_row = 2 * half_count
    rows = half_rows // CHUNKS
    for i, block_ref in enumerate((piece_ref, second_ref)):
        start = pl.multiple_of(place_ref[0] * half_rows + i * rows, rows)
        block_ref[:half_count] = feature_ref[:, :, pl.ds(start, rows)].reshape(half_count, rows)
        block_ref[half_count:first_row] = other_ref[:, i * rows : (i + 1) * rows]
    high, group = place_ref[2], place_ref[3]
    count = 8
    half = tower_ref.shape[0] // 2
    entries = 16
    planes = LANES // entries
    start = pl.multiple_of(group * count, count)
    lane = lax.broadcasted_iota(jnp.int32, (count, LANES), 1)
    sources = [
        tower_ref[high * half + f, pl.ds(start, count)].astype(jnp.float32) for f in range(half)
    ]
    query = query_ref[pl.ds(start, count)].astype(jnp.float32)
    bias = bias_ref[pl.ds(start, count)]
    first = bias.astype(jnp.bfloat16).astype(jnp.float32)
    second = (bias - first).astype(jnp.bfloat16).astype(jnp.float32)
    third = bias - first - second
    bias_lanes = jnp.where(
        lane == 96, first, jnp.where(lane == 97, second, jnp.where(lane == 98, third, 0.0))
    )
    bias_lanes = jnp.where(high == 0, bias_lanes, 0.0)
    for plane in range(planes):
        for tile in range(2):
            kept = bias_lanes if (tile == 1 and plane == 0) else jnp.zeros((count, LANES), jnp.float32)
            inside = [(f % 8, sources[f]) for f in range(half) if f // 8 == tile]
            if tile == 1:
                inside.append((5, query))
            for slot, source in inside:
                moved = pltpu.roll(source, ((slot - plane) * entries) % LANES, 1)
                kept = jnp.where((lane >= slot * entries) & (lane < (slot + 1) * entries), moved, kept)
            span = slice(tile * LANES, (tile + 1) * LANES)
            at = first_row + plane * count
            piece_ref[at : at + count, span] = kept.astype(jnp.bfloat16)


def stack_kernel(first_row, candidate_ref, *refs):
    blocks, out_ref = refs[:-1], refs[-1]
    planes = len(blocks)
    for source, block_ref in enumerate(blocks):
        for z in range(planes):
            at = first_row + z * 8
            out_ref[source * 8 : source * 8 + 8, z * WIDE : (z + 1) * WIDE] = block_ref[at : at + 8]
    units = planes * 8
    for t in range(out_ref.shape[1] // LANES):
        out_ref[units:, t * LANES : (t + 1) * LANES] = candidate_ref[t * 16 : (t + 1) * 16]


def pile_kernel(*refs):
    parts, out_ref, done = refs[:-2], refs[-2], refs[-1]
    copies = [
        pltpu.make_async_copy(part_ref, out_ref.at[i], done.at[i]) for i, part_ref in enumerate(parts)
    ]
    for copy in copies:
        copy.start()
    for copy in copies:
        copy.wait()


def loss_kernel(near, scale, place_ref, user_ref, target_ref, input_ref, *refs):
    sources = refs[:8]
    out_ref, weight_ref, candidate_ref, score_ref, done, candidate_done = refs[8:]
    _, small, units, width = weight_ref.shape
    for i in (0, 3, 1, 2, 4, 7, 5, 6):
        pltpu.make_async_copy(sources[i].at[:, :units], weight_ref.at[i], done.at[i]).start()
    copies = [
        pltpu.make_async_copy(sources[i].at[:, units:], candidate_ref.at[i], candidate_done.at[i])
        for i in range(4)
    ]
    for copy in copies:
        copy.start()
    core, plane, home = place_ref[0], place_ref[1], (place_ref[4], place_ref[5])
    planes = input_ref.shape[0]
    rows = user_ref.shape[0]
    contract = (((1,), (1,)), ((), ()))

    def inputs(which):
        at = pl.multiple_of(which * WIDE, WIDE)
        return jnp.concatenate([input_ref[z, :, pl.ds(at, WIDE)] for z in range(planes)], axis=1)

    def tower_step(n, gathered):
        owner, step = n // 2, n % 2
        spot = jnp.where(lax.rem(core + owner, 2) == 0, home[1], home[0])
        which = lax.rem(lax.rem(spot + step, 4) // 2 + core, 2)
        first, second = 4 * owner + step, 4 * owner + 3 - step
        for i in (first, second):
            pltpu.make_async_copy(weight_ref.at[i], weight_ref.at[i], done.at[i]).wait()
        a = weight_ref[first].reshape(small * units, width)
        b = weight_ref[second].reshape(small * units, width)
        pre = lax.dot_general(inputs(which), a, contract, preferred_element_type=jnp.float32)
        pre += lax.dot_general(inputs(1 - which), b, contract, preferred_element_type=jnp.float32)
        hidden = jnp.maximum(pre, 0.0).astype(jnp.bfloat16)
        tails = jnp.concatenate(
            [a[:, z * WIDE + LANES : (z + 1) * WIDE] for z in range(planes)], axis=1
        )
        return gathered + jnp.dot(hidden, tails, preferred_element_type=jnp.float32)

    gathered = lax.fori_loop(0, 4, tower_step, jnp.zeros((rows, planes * LANES), jnp.float32))
    lane = lax.broadcasted_iota(jnp.int32, (rows, LANES), 1)
    part = jnp.zeros((rows, LANES), jnp.float32)
    for z in range(planes):
        moved = pltpu.roll(gathered[:, z * LANES : (z + 1) * LANES], ((z - 5) * 16) % LANES, 1)
        part = jnp.where((lane >= z * 16) & (lane < (z + 1) * 16), moved, part)
    query = (part + user_ref[...].astype(jnp.float32)).astype(jnp.bfloat16)
    for copy in copies:
        copy.wait()
    lines = width // LANES
    count = lines * 16
    target = target_ref[:, :1]
    wide_lane = lax.broadcasted_iota(jnp.int32, (rows, count), 1)

    def score_step(number, state):
        picked, best = state
        far_offset = number ^ (number >> 1)
        for slot, near_offset in enumerate(near):
            rows_of = jnp.concatenate(
                [candidate_ref[number, slot, :, t * LANES : (t + 1) * LANES] for t in range(lines)],
                axis=0,
            )
            logits = (
                lax.dot_general(query, rows_of, contract, preferred_element_type=jnp.float32) * scale
            )
            outer = lax.rem(home[0] + jnp.where(core == 0, near_offset, far_offset), 4)
            inner = lax.rem(home[1] + jnp.where(core == 0, far_offset, near_offset), 4)
            base = (outer * 4 + inner) * count
            picked += jnp.where(wide_lane == target - base, logits, 0.0)
            best = jnp.maximum(best, logits)
            score_ref[number * 4 + slot] = logits
        return picked, best

    picked, best = lax.fori_loop(
        0,
        4,
        score_step,
        (jnp.zeros((rows, count), jnp.float32), jnp.full((rows, count), -1e30, jnp.float32)),
    )
    picked = jnp.sum(picked, axis=1, keepdims=True)
    best = jnp.max(best, axis=1, keepdims=True)

    def total_step(i, total):
        return total + jnp.exp(score_ref[i] - best)

    total = lax.fori_loop(0, score_ref.shape[0], total_step, jnp.zeros((rows, count), jnp.float32))
    total = jnp.sum(total, axis=1, keepdims=True)
    loss = best + jnp.log(total) - picked
    share = rows // CHUNKS
    row = lax.broadcasted_iota(jnp.int32, (rows, LANES), 0)
    spot = lax.rem(plane, LANES // share) * share
    for i in range(CHUNKS):
        mine = (row >= i * share) & (lane == row - i * share + spot)
        mine = mine & (row < (i + 1) * share)
        line = jnp.sum(jnp.where(mine, loss, 0.0), axis=0, keepdims=True)
        out_ref[:, i] = jnp.broadcast_to(line, (out_ref.shape[0], LANES))


def end_kernel(planes, lines_ref, out_ref):
    cores = lines_ref.shape[0] // planes
    groups = out_ref.shape[0] // (cores * CHUNKS)
    for c in range(cores):
        for i in range(CHUNKS):
            for g in range(groups):
                first = c * planes + g * (planes // groups)
                parts = [lines_ref[first + z, i : i + 1] for z in range(planes // groups)]
                at = (c * CHUNKS + i) * groups + g
                out_ref[at : at + 1] = functools.reduce(jnp.add, parts)


def as_column(values):
    return jnp.broadcast_to(values.reshape(-1, 1), (values.size, LANES))


def over_planes(x):
    return lax.all_to_all(x, "dim", split_axis=0, concat_axis=0, tiled=True)


def over_all(x):
    return lax.all_to_all(x, ("field", "dim"), split_axis=0, concat_axis=0, tiled=True)


def program(
    features,
    cross_weight,
    cross_bias,
    tower_weight,
    tower_bias,
    query_weight,
    user_vec,
    candidates,
    positive,
):
    core = lax.axis_index("field")
    plane = lax.axis_index("dim")
    planes = lax.axis_size("dim")
    home = [lax.axis_index(axis) for axis in BATCH]
    field_local, entry_local, row_count = features.shape
    half_rows = row_count // 2
    chunk_rows = half_rows // CHUNKS
    share = chunk_rows // planes
    near_spot = jnp.where(core == 0, home[0], home[1])
    far_spot = jnp.where(core == 0, home[1], home[0])
    place = jnp.stack(
        [core, plane, far_spot // 2, 2 * near_spot + far_spot % 2, home[0], home[1]]
    ).astype(jnp.int32)

    def swap(x):
        return shift(x, "field", 1)

    half_count = field_local * entry_local
    count = 2 * half_count
    theirs = pl.pallas_call(
        cut_kernel,
        out_shape=jax.ShapeDtypeStruct((half_count, half_rows), jnp.bfloat16),
        in_specs=[SMEM, VMEM],
        out_specs=VMEM,
        compiler_params=grant(4),
    )(place, features)
    fetched = swap(theirs)
    weights = cross_weight.transpose(0, 1, 3, 2, 4)
    biases = cross_bias.transpose(1, 0, 2)

    other_weights = swap(weights)
    other_bias = swap(biases)

    anchors = pl.pallas_call(
        pick_kernel,
        out_shape=[
            jax.ShapeDtypeStruct((count + 8 * planes, chunk_rows), jnp.bfloat16),
            jax.ShapeDtypeStruct((count, chunk_rows), jnp.bfloat16),
        ],
        in_specs=[SMEM] + [VMEM] * 5,
        out_specs=[VMEM] * 2,
        compiler_params=grant(6),
    )(place, features, fetched, tower_weight.transpose(1, 0, 2), as_column(tower_bias), query_weight)
    rings = [ring_gather(anchors[0], "dim", True), ring_gather(anchors[1], "dim", False)]
    width = planes * WIDE
    stack = pl.pallas_call(
        functools.partial(stack_kernel, count),
        out_shape=jax.ShapeDtypeStruct((8 * planes + 16, width), jnp.bfloat16),
        in_specs=[VMEM] * (1 + planes),
        out_specs=VMEM,
        compiler_params=grant(8),
    )(candidates, *[block for _, block in rings[0]])
    near_up = crosswise(stack, 1, False)
    near_down = crosswise(stack, -1, False)
    near_two = crosswise(stack, 2, False)
    near = (0, 3, 1, 2)
    block = pl.pallas_call(
        pile_kernel,
        out_shape=jax.ShapeDtypeStruct((4,) + stack.shape, stack.dtype),
        in_specs=[ANY] * 4,
        out_specs=ANY,
        scratch_shapes=[pltpu.SemaphoreType.DMA((4,))],
        compiler_params=grant(4),
    )(stack, near_up, near_down, near_two)
    far_down = crosswise(block, -1, True)
    far_up = crosswise(block, 1, True)
    far_two = crosswise(far_up, 1, True)
    own_arrays = [block, far_down, far_up, far_two]
    arrays = own_arrays + [swap(a) for a in own_arrays]
    for level in range(CROSS):
        matrix, bias = ordered_weight(level, place, weights, other_weights, biases, other_bias)
        results = []
        for i in range(CHUNKS):
            turn = i + 1 if level == CROSS - 1 else 0
            earlier = [results[-1][1]] if turn == 2 else []
            results.append(cross_layer(place, matrix, bias, anchors[i], rings[i], turn, earlier))
        if level < CROSS - 1:
            rings = [ring_gather(results[i][0], "dim", i % 2 == 0) for i in range(CHUNKS)]

    final = jnp.concatenate([result[0] for result in results], axis=1)
    final = final.reshape(2 * field_local, entry_local, half_rows)
    kept = final[:field_local]
    fetched = swap(final[field_local:])
    crossed = jnp.where(
        core == 0,
        jnp.concatenate([kept, fetched], axis=2),
        jnp.concatenate([fetched, kept], axis=2),
    )

    exchanged = over_planes(results[-1][1])
    starts = [core * half_rows + i * chunk_rows + plane * share for i in range(CHUNKS)]
    user_rows = jnp.concatenate([lax.dynamic_slice_in_dim(user_vec, s, share, 0) for s in starts])
    targets = jnp.concatenate([lax.dynamic_slice_in_dim(positive, s, share, 0) for s in starts])
    loss = pl.pallas_call(
        functools.partial(loss_kernel, near, 1.0 / math.sqrt(query_weight.shape[1])),
        out_shape=jax.ShapeDtypeStruct((2 * planes, CHUNKS, LANES), jnp.float32),
        in_specs=[SMEM] + [VMEM] * 3 + [ANY] * len(arrays),
        out_specs=VMEM,
        scratch_shapes=[
            pltpu.VMEM((len(arrays), 4, 8 * planes, width), jnp.bfloat16),
            pltpu.VMEM((4, 4, 16, width), jnp.bfloat16),
            pltpu.VMEM((16, CHUNKS * share, width // 8), jnp.float32),
            pltpu.SemaphoreType.DMA((len(arrays),)),
            pltpu.SemaphoreType.DMA((4,)),
        ],
        compiler_params=grant(20),
    )(place, user_rows, as_column(targets), exchanged, *arrays)
    lines = over_all(loss)
    losses = pl.pallas_call(
        functools.partial(end_kernel, planes),
        out_shape=jax.ShapeDtypeStruct((row_count // LANES, LANES), jnp.float32),
        in_specs=[VMEM],
        out_specs=VMEM,
        compiler_params=grant(4),
    )(lines)
    return (crossed, losses.reshape(row_count))


def solution(mesh):
    torus = Mesh(
        mesh.devices.reshape(4, 4, mesh.shape["field"], mesh.shape["dim"]),
        ("batch_0", "batch_1", "field", "dim"),
    )
    in_specs = (
        P("field", "dim", BATCH),
        P(None, "field", "dim", None, None),
        P(None, "field", "dim"),
        P(("field", "dim"), None, None),
        P(("field", "dim")),
        P(("field", "dim"), None),
        P(BATCH, None),
        P(BATCH, None),
        P(BATCH),
    )
    out_specs = (P("field", "dim", BATCH), P(BATCH))
    return jax.shard_map(program, mesh=torus, in_specs=in_specs, out_specs=out_specs, check_vma=False)
```

```python
import functools
import math

import jax
import jax.numpy as jnp
from jax import lax
from jax.experimental import pallas as pl
from jax.experimental.pallas import tpu as pltpu
from jax.sharding import Mesh
from jax.sharding import PartitionSpec as P


CROSS = 2
BATCH = ("batch_0", "batch_1")
CHUNKS = 2
LANES = 128
WIDE = 256
SMEM = pl.BlockSpec(memory_space=pltpu.SMEM)
VMEM = pl.BlockSpec(memory_space=pltpu.VMEM)
ANY = pl.BlockSpec(memory_space=pl.ANY)
HBM = pl.BlockSpec(memory_space=pltpu.HBM)


def grant(mib):
    return pltpu.CompilerParams(vmem_limit_bytes=mib * 1024 * 1024)


def shift(x, axis, step):
    length = lax.axis_size(axis)
    return lax.ppermute(x, axis, [(i, (i + step) % length) for i in range(length)])


def ring_gather(block, axis, forward):
    length = lax.axis_size(axis)
    up = length // 2 if forward else length - 1 - length // 2
    down = length - 1 - up
    found = [(0, block)]
    rising = falling = block
    for step in range(1, max(up, down) + 1):
        if step <= up:
            rising = shift(rising, axis, 1)
            found.append((-step, rising))
        if step <= down:
            falling = shift(falling, axis, -1)
            found.append((step, falling))
    return found


def crosswise(x, step, far):
    outer, inner = (lax.axis_size(axis) for axis in BATCH)
    pairs = []
    for a in range(outer):
        for b in range(inner):
            for core in range(2):
                if (core == 0) != far:
                    target = ((a + step) % outer, b)
                else:
                    target = (a, (b + step) % inner)
                pairs.append((2 * (a * inner + b) + core, 2 * (target[0] * inner + target[1]) + core))
    return lax.ppermute(x, BATCH + ("field",), pairs)


def order_kernel(level, place_ref, own_ref, other_ref, bias_ref, other_bias_ref, out_ref, column_ref):
    core = place_ref[0]
    _, outer, fields, entries, lanes = own_ref.shape
    rows = outer * entries
    half = fields // 2

    def step(k, _):
        for part in range(2):
            group = 2 * k + part
            high = (group >= half).astype(jnp.int32)
            source = lax.rem(core + high, 2) * half + group - high * half
            span = slice(part * lanes, (part + 1) * lanes)
            out_ref[k, :rows, span] = own_ref[0, :, source].reshape(rows, lanes)
            out_ref[k, rows:, span] = other_ref[0, :, source].reshape(rows, lanes)
        return 0

    lax.fori_loop(0, fields // 2, step, 0)
    line = lax.broadcasted_iota(jnp.int32, (entries, entries), 0)
    lane = lax.broadcasted_iota(jnp.int32, (entries, entries), 1)
    for side, side_ref in enumerate((bias_ref, other_bias_ref)):
        for f in range(outer):
            values = side_ref[f, level : level + 1, :]
            turned = jnp.sum(jnp.where(line == lane, values, 0.0), axis=1, keepdims=True)
            at = side * rows + f * entries
            column_ref[at : at + entries, :] = jnp.broadcast_to(turned, (entries, LANES))


def ordered_weight(level, place, own, other, bias, other_bias):
    _, outer, fields, entries, lanes = own.shape
    rows = 2 * outer * entries
    part = pl.BlockSpec((1, outer, fields, entries, lanes), lambda i: (level, 0, 0, 0, 0))
    whole = pl.BlockSpec(bias.shape, lambda i: (0, 0, 0))
    out_shape = (
        jax.ShapeDtypeStruct((fields // 2, rows, 2 * lanes), own.dtype),
        jax.ShapeDtypeStruct((rows, LANES), jnp.float32),
    )
    return pl.pallas_call(
        functools.partial(order_kernel, level),
        grid=(1,),
        out_shape=out_shape,
        in_specs=[SMEM, part, part, whole, whole],
        out_specs=(
            pl.BlockSpec(out_shape[0].shape, lambda i: (0, 0, 0)),
            pl.BlockSpec(out_shape[1].shape, lambda i: (0, 0)),
        ),
        compiler_params=grant(14),
    )(place, own, other, bias, other_bias)


def layer_kernel(offsets, turn, place_ref, weight_ref, bias_ref, anchor_ref, *refs):
    length = len(offsets)
    blocks, refs = refs[:length], refs[length:]
    plane = place_ref[1]
    if turn:
        whole_ref, turned_ref, keep_ref, send_ref, done = refs[-5:]
        outs = refs[-8:-5]
    else:
        outs, whole_ref = refs[:1], refs[1]
    fields, _, entries, rows = whole_ref.shape
    count = fields * entries
    for offset, block_ref in zip(offsets, blocks):
        source = lax.rem(plane + offset + length, length)
        whole_ref[:, source] = block_ref[:count].reshape(fields, entries, rows)
    weight = jnp.concatenate([weight_ref[k] for k in range(weight_ref.shape[0])], axis=1)
    inputs = whole_ref[...].reshape(length * count, rows)
    product = jnp.dot(weight, inputs, preferred_element_type=jnp.float32) + bias_ref[:, :1]
    anchor = anchor_ref[:count].astype(jnp.float32)
    current = blocks[0][:count].astype(jnp.float32)
    result = (anchor * product + current).astype(jnp.bfloat16)
    if not turn:
        outs[0][...] = result
        return
    turn_ref, crossed_ref, other_ref = outs
    keep_ref[...] = result[: count // 2].reshape(keep_ref.shape)
    send_ref[...] = result[count // 2 :]
    half = other_ref.shape[1]
    first = (turn - 1) * rows
    start = pl.multiple_of(place_ref[0] * half + first, rows)
    copies = [
        pltpu.make_async_copy(keep_ref, crossed_ref.at[:, :, pl.ds(start, rows)], done.at[0]),
        pltpu.make_async_copy(send_ref, other_ref.at[:, pl.ds(first, rows)], done.at[1]),
    ]
    for copy in copies:
        copy.start()
    halves = result.reshape(2, count // 2, rows).astype(jnp.float32)
    spare = WIDE - count // 2
    share = rows // length
    line = lax.broadcasted_iota(jnp.int32, (spare, rows), 0)
    ones = jnp.where((line >= 16) & (line < 19), 1.0, 0.0)
    for h in range(2):
        turned = jnp.concatenate([halves[h], ones], axis=0).T.astype(jnp.bfloat16)
        turned_ref[h] = turned.reshape(length, share, WIDE)
        span = slice(h * WIDE, (h + 1) * WIDE)
        target = turn_ref.at[:, pl.ds((turn - 1) * share, share), span]
        copies.append(pltpu.make_async_copy(turned_ref.at[h], target, done.at[2 + h]))
        copies[-1].start()
    for copy in copies:
        copy.wait()


def cross_layer(place, matrix, bias, anchor, found, turn, earlier):
    offsets = tuple(offset for offset, _ in found)
    blocks = [block for _, block in found]
    count, rows = matrix.shape[1], anchor.shape[1]
    planes = len(blocks)
    out_shape = [jax.ShapeDtypeStruct((count, rows), jnp.bfloat16)]
    scratch = [pltpu.VMEM((count // 16, planes, 16, rows), jnp.bfloat16)]
    if turn:
        fields = count // 32
        out_shape = [
            pltpu.HBM((planes, CHUNKS * rows // planes, 2 * WIDE), jnp.bfloat16),
            pltpu.HBM((fields, 16, 2 * CHUNKS * rows), jnp.bfloat16),
            pltpu.HBM((count // 2, CHUNKS * rows), jnp.bfloat16),
        ]
        scratch += [
            pltpu.VMEM((2, planes, rows // planes, WIDE), jnp.bfloat16),
            pltpu.VMEM((fields, 16, rows), jnp.bfloat16),
            pltpu.VMEM((count // 2, rows), jnp.bfloat16),
            pltpu.SemaphoreType.DMA((4,)),
        ]
    base = 4 + planes
    return pl.pallas_call(
        functools.partial(layer_kernel, offsets, turn),
        out_shape=out_shape,
        in_specs=[SMEM] + [VMEM] * (3 + planes) + [HBM] * len(earlier),
        out_specs=[HBM] * 3 if turn else [VMEM],
        input_output_aliases={base + i: i for i in range(len(earlier))},
        scratch_shapes=scratch,
        compiler_params=grant(14),
    )(place, matrix, bias, anchor, *blocks, *earlier)


def in_hbm(x):
    return pltpu.with_memory_space_constraint(x, pltpu.HBM)


def fill_kernel(place_ref, fetched_ref, given_ref, crossed_ref, done):
    half = fetched_ref.shape[2]
    start = pl.multiple_of((1 - place_ref[0]) * half, half)
    copy = pltpu.make_async_copy(fetched_ref, crossed_ref.at[:, :, pl.ds(start, half)], done)
    copy.start()
    copy.wait()


def cut_kernel(place_ref, feature_ref, theirs_ref, mine_ref, whole_ref, done):
    copy = pltpu.make_async_copy(feature_ref, whole_ref, done)
    copy.start()
    copy.wait()
    count, half = theirs_ref.shape
    for side, out_ref in enumerate((mine_ref, theirs_ref)):
        start = pl.multiple_of(jnp.abs(side - place_ref[0]) * half, half)
        out_ref[...] = whole_ref[:, :, pl.ds(start, half)].reshape(count, half)


def pick_kernel(
    place_ref, all_bias_ref, tower_ref, query_ref, piece_ref, part_ref, row_ref, bias_ref, done
):
    high, group = place_ref[2], place_ref[3]
    half, count, _ = part_ref.shape
    entries = 16
    planes = LANES // entries
    start = pl.multiple_of(group * count, count)
    copies = [
        pltpu.make_async_copy(
            tower_ref.at[pl.ds(high * half, half), pl.ds(start, count)], part_ref, done.at[0]
        ),
        pltpu.make_async_copy(query_ref.at[pl.ds(start, count)], row_ref, done.at[1]),
        pltpu.make_async_copy(all_bias_ref, bias_ref, done.at[2]),
    ]
    for copy in copies:
        copy.start()
    for copy in copies:
        copy.wait()
    lane = lax.broadcasted_iota(jnp.int32, (count, LANES), 1)
    line = lax.broadcasted_iota(jnp.int32, (count, LANES), 0)
    bias = jnp.zeros((count, LANES), jnp.float32)
    for u in range(count):
        bias = jnp.where(line == u, bias_ref[start + u], bias)
    sources = [part_ref[f].astype(jnp.float32) for f in range(half)]
    query = row_ref[...].astype(jnp.float32)
    first = bias.astype(jnp.bfloat16).astype(jnp.float32)
    second = (bias - first).astype(jnp.bfloat16).astype(jnp.float32)
    third = bias - first - second
    bias_lanes = jnp.where(
        lane == 96, first, jnp.where(lane == 97, second, jnp.where(lane == 98, third, 0.0))
    )
    bias_lanes = jnp.where(high == 0, bias_lanes, 0.0)
    for plane in range(planes):
        for tile in range(2):
            kept = bias_lanes if (tile == 1 and plane == 0) else jnp.zeros((count, LANES), jnp.float32)
            inside = [(f % 8, sources[f]) for f in range(half) if f // 8 == tile]
            if tile == 1:
                inside.append((5, query))
            for slot, source in inside:
                moved = pltpu.roll(source, ((slot - plane) * entries) % LANES, 1)
                kept = jnp.where((lane >= slot * entries) & (lane < (slot + 1) * entries), moved, kept)
            span = slice(tile * LANES, (tile + 1) * LANES)
            piece_ref[plane * count : (plane + 1) * count, span] = kept.astype(jnp.bfloat16)


def join_kernel(mine_ref, other_ref, piece_ref, first_ref, second_ref):
    half_count, half_rows = other_ref.shape
    rows = half_rows // CHUNKS
    for i, block_ref in enumerate((first_ref, second_ref)):
        span = slice(i * rows, (i + 1) * rows)
        block_ref[:half_count] = mine_ref[:, span]
        block_ref[half_count : 2 * half_count] = other_ref[:, span]
    first_ref[2 * half_count :] = piece_ref[...]


def stack_kernel(first_row, candidate_ref, *refs):
    blocks, out_ref = refs[:-1], refs[-1]
    planes = len(blocks)
    for source, block_ref in enumerate(blocks):
        for z in range(planes):
            at = first_row + z * 8
            out_ref[source * 8 : source * 8 + 8, z * WIDE : (z + 1) * WIDE] = block_ref[at : at + 8]
    units = planes * 8
    for t in range(out_ref.shape[1] // LANES):
        out_ref[units:, t * LANES : (t + 1) * LANES] = candidate_ref[t * 16 : (t + 1) * 16]


def pile_kernel(*refs):
    parts, out_ref, done = refs[:-2], refs[-2], refs[-1]
    copies = [
        pltpu.make_async_copy(part_ref, out_ref.at[i], done.at[i]) for i, part_ref in enumerate(parts)
    ]
    for copy in copies:
        copy.start()
    for copy in copies:
        copy.wait()


def loss_kernel(near, scale, place_ref, all_user_ref, all_target_ref, input_ref, *refs):
    sources = refs[:8]
    out_ref, weight_ref, candidate_ref, score_ref, user_ref, done, candidate_done, user_done = refs[8:]
    _, small, units, width = weight_ref.shape
    for i in (0, 3, 1, 2, 4, 7, 5, 6):
        pltpu.make_async_copy(sources[i].at[:, :units], weight_ref.at[i], done.at[i]).start()
    copies = [
        pltpu.make_async_copy(sources[i].at[:, units:], candidate_ref.at[i], candidate_done.at[i])
        for i in range(4)
    ]
    for copy in copies:
        copy.start()
    core, plane, home = place_ref[0], place_ref[1], (place_ref[4], place_ref[5])
    planes, rows, _ = input_ref.shape
    share = rows // CHUNKS
    targets, users = [], []
    for i in range(CHUNKS):
        start = (core * CHUNKS + i) * (planes * share) + plane * share
        start = pl.multiple_of(start, share)
        users.append(
            pltpu.make_async_copy(
                all_user_ref.at[pl.ds(start, share)],
                user_ref.at[i * share : (i + 1) * share],
                user_done.at[i],
            )
        )
        users[-1].start()
        values = jnp.broadcast_to(all_target_ref[pl.ds(start // LANES, 1)], (share, LANES))
        line = lax.broadcasted_iota(jnp.int32, (share, LANES), 0) + lax.rem(start, LANES)
        spots = lax.broadcasted_iota(jnp.int32, (share, LANES), 1)
        targets.append(jnp.sum(jnp.where(line == spots, values, 0), axis=1, keepdims=True))
    target = jnp.concatenate(targets, axis=0)
    contract = (((1,), (1,)), ((), ()))

    def inputs(which):
        at = pl.multiple_of(which * WIDE, WIDE)
        return jnp.concatenate([input_ref[z, :, pl.ds(at, WIDE)] for z in range(planes)], axis=1)

    def tower_step(n, gathered):
        owner, step = n // 2, n % 2
        spot = jnp.where(lax.rem(core + owner, 2) == 0, home[1], home[0])
        which = lax.rem(lax.rem(spot + step, 4) // 2 + core, 2)
        first, second = 4 * owner + step, 4 * owner + 3 - step
        for i in (first, second):
            pltpu.make_async_copy(weight_ref.at[i], weight_ref.at[i], done.at[i]).wait()
        a = weight_ref[first].reshape(small * units, width)
        b = weight_ref[second].reshape(small * units, width)
        pre = lax.dot_general(inputs(which), a, contract, preferred_element_type=jnp.float32)
        pre += lax.dot_general(inputs(1 - which), b, contract, preferred_element_type=jnp.float32)
        hidden = jnp.maximum(pre, 0.0).astype(jnp.bfloat16)
        tails = jnp.concatenate(
            [a[:, z * WIDE + LANES : (z + 1) * WIDE] for z in range(planes)], axis=1
        )
        return gathered + jnp.dot(hidden, tails, preferred_element_type=jnp.float32)

    gathered = lax.fori_loop(0, 4, tower_step, jnp.zeros((rows, planes * LANES), jnp.float32))
    lane = lax.broadcasted_iota(jnp.int32, (rows, LANES), 1)
    part = jnp.zeros((rows, LANES), jnp.float32)
    for z in range(planes):
        moved = pltpu.roll(gathered[:, z * LANES : (z + 1) * LANES], ((z - 5) * 16) % LANES, 1)
        part = jnp.where((lane >= z * 16) & (lane < (z + 1) * 16), moved, part)
    for copy in users:
        copy.wait()
    query = (part + user_ref[...].astype(jnp.float32)).astype(jnp.bfloat16)
    for copy in copies:
        copy.wait()
    lines = width // LANES
    count = lines * 16
    wide_lane = lax.broadcasted_iota(jnp.int32, (rows, count), 1)

    def score_step(number, state):
        picked, best = state
        far_offset = number ^ (number >> 1)
        for slot, near_offset in enumerate(near):
            rows_of = jnp.concatenate(
                [candidate_ref[number, slot, :, t * LANES : (t + 1) * LANES] for t in range(lines)],
                axis=0,
            )
            logits = (
                lax.dot_general(query, rows_of, contract, preferred_element_type=jnp.float32) * scale
            )
            outer = lax.rem(home[0] + jnp.where(core == 0, near_offset, far_offset), 4)
            inner = lax.rem(home[1] + jnp.where(core == 0, far_offset, near_offset), 4)
            base = (outer * 4 + inner) * count
            picked += jnp.where(wide_lane == target - base, logits, 0.0)
            best = jnp.maximum(best, logits)
            score_ref[number * 4 + slot] = logits
        return picked, best

    picked, best = lax.fori_loop(
        0,
        4,
        score_step,
        (jnp.zeros((rows, count), jnp.float32), jnp.full((rows, count), -1e30, jnp.float32)),
    )
    picked = jnp.sum(picked, axis=1, keepdims=True)
    best = jnp.max(best, axis=1, keepdims=True)

    def total_step(i, total):
        return total + jnp.exp(score_ref[i] - best)

    total = lax.fori_loop(0, score_ref.shape[0], total_step, jnp.zeros((rows, count), jnp.float32))
    total = jnp.sum(total, axis=1, keepdims=True)
    loss = best + jnp.log(total) - picked
    row = lax.broadcasted_iota(jnp.int32, (rows, LANES), 0)
    spot = lax.rem(plane, LANES // share) * share
    for i in range(CHUNKS):
        mine = (row >= i * share) & (lane == row - i * share + spot)
        mine = mine & (row < (i + 1) * share)
        line = jnp.sum(jnp.where(mine, loss, 0.0), axis=0, keepdims=True)
        out_ref[:, i] = jnp.broadcast_to(line, (out_ref.shape[0], LANES))


def end_kernel(planes, lines_ref, out_ref):
    cores = lines_ref.shape[0] // planes
    groups = out_ref.shape[0] // (cores * CHUNKS)
    for c in range(cores):
        for i in range(CHUNKS):
            for g in range(groups):
                first = c * planes + g * (planes // groups)
                parts = [lines_ref[first + z, i : i + 1] for z in range(planes // groups)]
                at = (c * CHUNKS + i) * groups + g
                out_ref[at : at + 1] = functools.reduce(jnp.add, parts)


def over_planes(x):
    return lax.all_to_all(x, "dim", split_axis=0, concat_axis=0, tiled=True)


def over_all(x):
    return lax.all_to_all(x, ("field", "dim"), split_axis=0, concat_axis=0, tiled=True)


def program(
    features,
    cross_weight,
    cross_bias,
    tower_weight,
    tower_bias,
    query_weight,
    user_vec,
    candidates,
    positive,
):
    core = lax.axis_index("field")
    plane = lax.axis_index("dim")
    planes = lax.axis_size("dim")
    home = [lax.axis_index(axis) for axis in BATCH]
    field_local, entry_local, row_count = features.shape
    half_rows = row_count // 2
    chunk_rows = half_rows // CHUNKS
    share = chunk_rows // planes
    near_spot = jnp.where(core == 0, home[0], home[1])
    far_spot = jnp.where(core == 0, home[1], home[0])
    place = jnp.stack(
        [core, plane, far_spot // 2, 2 * near_spot + far_spot % 2, home[0], home[1]]
    ).astype(jnp.int32)

    def swap(x):
        return shift(x, "field", 1)

    half_count = field_local * entry_local
    count = 2 * half_count
    theirs, mine = pl.pallas_call(
        cut_kernel,
        out_shape=[jax.ShapeDtypeStruct((half_count, half_rows), jnp.bfloat16)] * 2,
        in_specs=[SMEM, HBM],
        out_specs=[VMEM] * 2,
        scratch_shapes=[pltpu.VMEM(features.shape, jnp.bfloat16), pltpu.SemaphoreType.DMA],
        compiler_params=grant(4),
    )(place, in_hbm(features))
    fetched = swap(theirs)
    weights = cross_weight.transpose(0, 1, 3, 2, 4)
    biases = cross_bias.transpose(1, 0, 2)

    other_weights = swap(weights)
    other_bias = swap(biases)

    piece = pl.pallas_call(
        pick_kernel,
        out_shape=jax.ShapeDtypeStruct((8 * planes, WIDE), jnp.bfloat16),
        in_specs=[SMEM, HBM, HBM, HBM],
        out_specs=VMEM,
        scratch_shapes=[
            pltpu.VMEM((field_local, 8, LANES), jnp.bfloat16),
            pltpu.VMEM((8, LANES), jnp.bfloat16),
            pltpu.SMEM(tower_bias.shape, jnp.float32),
            pltpu.SemaphoreType.DMA((3,)),
        ],
        compiler_params=grant(2),
    )(place, in_hbm(tower_bias), in_hbm(tower_weight.transpose(1, 0, 2)), in_hbm(query_weight))
    anchors = pl.pallas_call(
        join_kernel,
        out_shape=[
            jax.ShapeDtypeStruct((count + 8 * planes, chunk_rows), jnp.bfloat16),
            jax.ShapeDtypeStruct((count, chunk_rows), jnp.bfloat16),
        ],
        in_specs=[VMEM] * 3,
        out_specs=[VMEM] * 2,
        compiler_params=grant(4),
    )(mine, fetched, piece)
    rings = [ring_gather(anchors[0], "dim", True), ring_gather(anchors[1], "dim", False)]
    width = planes * WIDE
    stack = pl.pallas_call(
        functools.partial(stack_kernel, count),
        out_shape=jax.ShapeDtypeStruct((8 * planes + 16, width), jnp.bfloat16),
        in_specs=[VMEM] * (1 + planes),
        out_specs=VMEM,
        compiler_params=grant(8),
    )(candidates, *[block for _, block in rings[0]])
    near_up = crosswise(stack, 1, False)
    near_down = crosswise(stack, -1, False)
    near_two = crosswise(stack, 2, False)
    near = (0, 3, 1, 2)
    block = pl.pallas_call(
        pile_kernel,
        out_shape=jax.ShapeDtypeStruct((4,) + stack.shape, stack.dtype),
        in_specs=[ANY] * 4,
        out_specs=ANY,
        scratch_shapes=[pltpu.SemaphoreType.DMA((4,))],
        compiler_params=grant(4),
    )(stack, near_up, near_down, near_two)
    far_down = crosswise(block, -1, True)
    far_up = crosswise(block, 1, True)
    far_two = crosswise(far_up, 1, True)
    own_arrays = [block, far_down, far_up, far_two]
    arrays = own_arrays + [swap(a) for a in own_arrays]
    for level in range(CROSS):
        matrix, bias = ordered_weight(level, place, weights, other_weights, biases, other_bias)
        results = []
        for i in range(CHUNKS):
            turn = i + 1 if level == CROSS - 1 else 0
            earlier = results[-1] if turn == 2 else []
            results.append(cross_layer(place, matrix, bias, anchors[i], rings[i], turn, earlier))
        if level < CROSS - 1:
            rings = [ring_gather(results[i][0], "dim", i % 2 == 0) for i in range(CHUNKS)]

    exchanged, partly, other_half = results[-1]
    exchanged = over_planes(exchanged)
    fetched = swap(other_half).reshape(field_local, entry_local, half_rows)
    crossed = pl.pallas_call(
        fill_kernel,
        out_shape=jax.ShapeDtypeStruct(partly.shape, partly.dtype),
        in_specs=[SMEM, VMEM, HBM],
        out_specs=HBM,
        input_output_aliases={2: 0},
        scratch_shapes=[pltpu.SemaphoreType.DMA],
        compiler_params=grant(2),
    )(place, fetched, partly)

    loss = pl.pallas_call(
        functools.partial(loss_kernel, near, 1.0 / math.sqrt(query_weight.shape[1])),
        out_shape=jax.ShapeDtypeStruct((2 * planes, CHUNKS, LANES), jnp.float32),
        in_specs=[SMEM, HBM, VMEM, VMEM] + [ANY] * len(arrays),
        out_specs=VMEM,
        scratch_shapes=[
            pltpu.VMEM((len(arrays), 4, 8 * planes, width), jnp.bfloat16),
            pltpu.VMEM((4, 4, 16, width), jnp.bfloat16),
            pltpu.VMEM((16, CHUNKS * share, width // 8), jnp.float32),
            pltpu.VMEM((CHUNKS * share, LANES), jnp.bfloat16),
            pltpu.SemaphoreType.DMA((len(arrays),)),
            pltpu.SemaphoreType.DMA((4,)),
            pltpu.SemaphoreType.DMA((CHUNKS,)),
        ],
        compiler_params=grant(20),
    )(place, user_vec, positive.reshape(-1, LANES), exchanged, *arrays)
    lines = over_all(loss)
    losses = pl.pallas_call(
        functools.partial(end_kernel, planes),
        out_shape=jax.ShapeDtypeStruct((row_count // LANES, LANES), jnp.float32),
        in_specs=[VMEM],
        out_specs=VMEM,
        compiler_params=grant(4),
    )(lines)
    return (crossed, losses.reshape(row_count))


def solution(mesh):
    torus = Mesh(
        mesh.devices.reshape(4, 4, mesh.shape["field"], mesh.shape["dim"]),
        ("batch_0", "batch_1", "field", "dim"),
    )
    in_specs = (
        P("field", "dim", BATCH),
        P(None, "field", "dim", None, None),
        P(None, "field", "dim"),
        P(("field", "dim"), None, None),
        P(("field", "dim")),
        P(("field", "dim"), None),
        P(BATCH, None),
        P(BATCH, None),
        P(BATCH),
    )
    out_specs = (P("field", "dim", BATCH), P(BATCH))
    return jax.shard_map(program, mesh=torus, in_specs=in_specs, out_specs=out_specs, check_vma=False)
```

```python
import functools
import math

import jax
import jax.numpy as jnp
from jax import lax
from jax.experimental import pallas as pl
from jax.experimental.pallas import tpu as pltpu
from jax.sharding import Mesh
from jax.sharding import PartitionSpec as P


CROSS = 2
BATCH = ("batch_0", "batch_1")
CHUNKS = 2
LANES = 128
WIDE = 256
SMEM = pl.BlockSpec(memory_space=pltpu.SMEM)
VMEM = pl.BlockSpec(memory_space=pltpu.VMEM)
ANY = pl.BlockSpec(memory_space=pl.ANY)
HBM = pl.BlockSpec(memory_space=pltpu.HBM)


def grant(mib):
    return pltpu.CompilerParams(vmem_limit_bytes=mib * 1024 * 1024)


def shift(x, axis, step):
    length = lax.axis_size(axis)
    return lax.ppermute(x, axis, [(i, (i + step) % length) for i in range(length)])


def ring_gather(block, axis, forward):
    length = lax.axis_size(axis)
    up = length // 2 if forward else length - 1 - length // 2
    down = length - 1 - up
    found = [(0, block)]
    rising = falling = block
    for step in range(1, max(up, down) + 1):
        if step <= up:
            rising = shift(rising, axis, 1)
            found.append((-step, rising))
        if step <= down:
            falling = shift(falling, axis, -1)
            found.append((step, falling))
    return found


def crosswise(x, step, far):
    outer, inner = (lax.axis_size(axis) for axis in BATCH)
    pairs = []
    for a in range(outer):
        for b in range(inner):
            for core in range(2):
                if (core == 0) != far:
                    target = ((a + step) % outer, b)
                else:
                    target = (a, (b + step) % inner)
                pairs.append((2 * (a * inner + b) + core, 2 * (target[0] * inner + target[1]) + core))
    return lax.ppermute(x, BATCH + ("field",), pairs)


def order_kernel(level, place_ref, own_ref, other_ref, bias_ref, other_bias_ref, out_ref, column_ref):
    core = place_ref[0]
    _, outer, fields, entries, lanes = own_ref.shape
    rows = outer * entries
    half = fields // 2

    def step(k, _):
        for part in range(2):
            group = 2 * k + part
            high = (group >= half).astype(jnp.int32)
            source = lax.rem(core + high, 2) * half + group - high * half
            span = slice(part * lanes, (part + 1) * lanes)
            out_ref[k, :rows, span] = own_ref[0, :, source].reshape(rows, lanes)
            out_ref[k, rows:, span] = other_ref[0, :, source].reshape(rows, lanes)
        return 0

    lax.fori_loop(0, fields // 2, step, 0)
    line = lax.broadcasted_iota(jnp.int32, (entries, entries), 0)
    lane = lax.broadcasted_iota(jnp.int32, (entries, entries), 1)
    for side, side_ref in enumerate((bias_ref, other_bias_ref)):
        for f in range(outer):
            values = side_ref[f, level : level + 1, :]
            turned = jnp.sum(jnp.where(line == lane, values, 0.0), axis=1, keepdims=True)
            at = side * rows + f * entries
            column_ref[at : at + entries, :] = jnp.broadcast_to(turned, (entries, LANES))


def ordered_weight(level, place, own, other, bias, other_bias):
    _, outer, fields, entries, lanes = own.shape
    rows = 2 * outer * entries
    part = pl.BlockSpec((1, outer, fields, entries, lanes), lambda i: (level, 0, 0, 0, 0))
    whole = pl.BlockSpec(bias.shape, lambda i: (0, 0, 0))
    out_shape = (
        jax.ShapeDtypeStruct((fields // 2, rows, 2 * lanes), own.dtype),
        jax.ShapeDtypeStruct((rows, LANES), jnp.float32),
    )
    return pl.pallas_call(
        functools.partial(order_kernel, level),
        grid=(1,),
        out_shape=out_shape,
        in_specs=[SMEM, part, part, whole, whole],
        out_specs=(
            pl.BlockSpec(out_shape[0].shape, lambda i: (0, 0, 0)),
            pl.BlockSpec(out_shape[1].shape, lambda i: (0, 0)),
        ),
        compiler_params=grant(14),
    )(place, own, other, bias, other_bias)


def layer_kernel(offsets, turn, place_ref, weight_ref, bias_ref, anchor_ref, *refs):
    length = len(offsets)
    blocks, refs = refs[:length], refs[length:]
    plane = place_ref[1]
    if turn:
        whole_ref, turned_ref, keep_ref, send_ref, done = refs[-5:]
        outs = refs[-8:-5]
    else:
        outs, whole_ref = refs[:1], refs[1]
    fields, _, entries, rows = whole_ref.shape
    count = fields * entries
    for offset, block_ref in zip(offsets, blocks):
        source = lax.rem(plane + offset + length, length)
        whole_ref[:, source] = block_ref[:count].reshape(fields, entries, rows)
    weight = jnp.concatenate([weight_ref[k] for k in range(weight_ref.shape[0])], axis=1)
    inputs = whole_ref[...].reshape(length * count, rows)
    product = jnp.dot(weight, inputs, preferred_element_type=jnp.float32) + bias_ref[:, :1]
    anchor = anchor_ref[:count].astype(jnp.float32)
    current = blocks[0][:count].astype(jnp.float32)
    result = (anchor * product + current).astype(jnp.bfloat16)
    if not turn:
        outs[0][...] = result
        return
    turn_ref, crossed_ref, other_ref = outs
    keep_ref[...] = result[: count // 2].reshape(keep_ref.shape)
    send_ref[...] = result[count // 2 :]
    half = other_ref.shape[1]
    first = (turn - 1) * rows
    start = pl.multiple_of(place_ref[0] * half + first, rows)
    copies = [
        pltpu.make_async_copy(keep_ref, crossed_ref.at[:, :, pl.ds(start, rows)], done.at[0]),
        pltpu.make_async_copy(send_ref, other_ref.at[:, pl.ds(first, rows)], done.at[1]),
    ]
    for copy in copies:
        copy.start()
    halves = result.reshape(2, count // 2, rows).astype(jnp.float32)
    spare = WIDE - count // 2
    share = rows // length
    line = lax.broadcasted_iota(jnp.int32, (spare, rows), 0)
    ones = jnp.where((line >= 16) & (line < 19), 1.0, 0.0)
    for h in range(2):
        turned = jnp.concatenate([halves[h], ones], axis=0).T.astype(jnp.bfloat16)
        turned_ref[h] = turned.reshape(length, share, WIDE)
        span = slice(h * WIDE, (h + 1) * WIDE)
        target = turn_ref.at[:, pl.ds((turn - 1) * share, share), span]
        copies.append(pltpu.make_async_copy(turned_ref.at[h], target, done.at[2 + h]))
        copies[-1].start()
    for copy in copies:
        copy.wait()


def cross_layer(place, matrix, bias, anchor, found, turn, earlier):
    offsets = tuple(offset for offset, _ in found)
    blocks = [block for _, block in found]
    count, rows = matrix.shape[1], anchor.shape[1]
    planes = len(blocks)
    out_shape = [jax.ShapeDtypeStruct((count, rows), jnp.bfloat16)]
    scratch = [pltpu.VMEM((count // 16, planes, 16, rows), jnp.bfloat16)]
    if turn:
        fields = count // 32
        out_shape = [
            pltpu.HBM((planes, CHUNKS * rows // planes, 2 * WIDE), jnp.bfloat16),
            pltpu.HBM((fields, 16, 2 * CHUNKS * rows), jnp.bfloat16),
            pltpu.HBM((count // 2, CHUNKS * rows), jnp.bfloat16),
        ]
        scratch += [
            pltpu.VMEM((2, planes, rows // planes, WIDE), jnp.bfloat16),
            pltpu.VMEM((fields, 16, rows), jnp.bfloat16),
            pltpu.VMEM((count // 2, rows), jnp.bfloat16),
            pltpu.SemaphoreType.DMA((4,)),
        ]
    base = 4 + planes
    return pl.pallas_call(
        functools.partial(layer_kernel, offsets, turn),
        out_shape=out_shape,
        in_specs=[SMEM] + [VMEM] * (3 + planes) + [HBM] * len(earlier),
        out_specs=[HBM] * 3 if turn else [VMEM],
        input_output_aliases={base + i: i for i in range(len(earlier))},
        scratch_shapes=scratch,
        compiler_params=grant(14),
    )(place, matrix, bias, anchor, *blocks, *earlier)


def in_hbm(x):
    return pltpu.with_memory_space_constraint(x, pltpu.HBM)


def fill_kernel(place_ref, fetched_ref, given_ref, crossed_ref, done):
    half = fetched_ref.shape[2]
    start = pl.multiple_of((1 - place_ref[0]) * half, half)
    copy = pltpu.make_async_copy(fetched_ref, crossed_ref.at[:, :, pl.ds(start, half)], done)
    copy.start()
    copy.wait()


def cut_kernel(place_ref, feature_ref, theirs_ref, mine_ref, whole_ref, done):
    copy = pltpu.make_async_copy(feature_ref, whole_ref, done)
    copy.start()
    copy.wait()
    count, half = theirs_ref.shape
    for side, out_ref in enumerate((mine_ref, theirs_ref)):
        start = pl.multiple_of(jnp.abs(side - place_ref[0]) * half, half)
        out_ref[...] = whole_ref[:, :, pl.ds(start, half)].reshape(count, half)


def pick_kernel(
    place_ref, all_bias_ref, tower_ref, query_ref, piece_ref, part_ref, row_ref, bias_ref, done
):
    high, group = place_ref[2], place_ref[3]
    half, count, _ = part_ref.shape
    entries = 16
    planes = LANES // entries
    start = pl.multiple_of(group * count, count)
    copies = [
        pltpu.make_async_copy(
            tower_ref.at[pl.ds(high * half, half), pl.ds(start, count)], part_ref, done.at[0]
        ),
        pltpu.make_async_copy(query_ref.at[pl.ds(start, count)], row_ref, done.at[1]),
        pltpu.make_async_copy(all_bias_ref, bias_ref, done.at[2]),
    ]
    for copy in copies:
        copy.start()
    for copy in copies:
        copy.wait()
    lane = lax.broadcasted_iota(jnp.int32, (count, LANES), 1)
    line = lax.broadcasted_iota(jnp.int32, (count, LANES), 0)
    bias = jnp.zeros((count, LANES), jnp.float32)
    for u in range(count):
        bias = jnp.where(line == u, bias_ref[start + u], bias)
    sources = [part_ref[f].astype(jnp.float32) for f in range(half)]
    query = row_ref[...].astype(jnp.float32)
    first = bias.astype(jnp.bfloat16).astype(jnp.float32)
    second = (bias - first).astype(jnp.bfloat16).astype(jnp.float32)
    third = bias - first - second
    bias_lanes = jnp.where(
        lane == 96, first, jnp.where(lane == 97, second, jnp.where(lane == 98, third, 0.0))
    )
    bias_lanes = jnp.where(high == 0, bias_lanes, 0.0)
    for plane in range(planes):
        for tile in range(2):
            kept = bias_lanes if (tile == 1 and plane == 0) else jnp.zeros((count, LANES), jnp.float32)
            inside = [(f % 8, sources[f]) for f in range(half) if f // 8 == tile]
            if tile == 1:
                inside.append((5, query))
            for slot, source in inside:
                moved = pltpu.roll(source, ((slot - plane) * entries) % LANES, 1)
                kept = jnp.where((lane >= slot * entries) & (lane < (slot + 1) * entries), moved, kept)
            span = slice(tile * LANES, (tile + 1) * LANES)
            piece_ref[plane * count : (plane + 1) * count, span] = kept.astype(jnp.bfloat16)


def join_kernel(mine_ref, other_ref, piece_ref, first_ref, second_ref):
    half_count, half_rows = other_ref.shape
    rows = half_rows // CHUNKS
    for i, block_ref in enumerate((first_ref, second_ref)):
        span = slice(i * rows, (i + 1) * rows)
        block_ref[:half_count] = mine_ref[:, span]
        block_ref[half_count : 2 * half_count] = other_ref[:, span]
    first_ref[2 * half_count :] = piece_ref[...]


def stack_kernel(first_row, place_ref, candidate_ref, *refs):
    blocks, out_ref = refs[:-1], refs[-1]
    planes = len(blocks)
    for source, block_ref in enumerate(blocks):
        for z in range(planes):
            at = first_row + z * 8
            out_ref[source * 8 : source * 8 + 8, z * WIDE : (z + 1) * WIDE] = block_ref[at : at + 8]
    units = planes * 8
    lines = out_ref.shape[1] // LANES
    for t in range(lines):
        at = pl.multiple_of(place_ref[0] * (8 * lines) + t * 8, 8)
        out_ref[units:, t * LANES : (t + 1) * LANES] = candidate_ref[pl.ds(at, 8)]


def pile_kernel(*refs):
    parts, out_ref, done = refs[:-2], refs[-2], refs[-1]
    copies = [
        pltpu.make_async_copy(part_ref, out_ref.at[i], done.at[i]) for i, part_ref in enumerate(parts)
    ]
    for copy in copies:
        copy.start()
    for copy in copies:
        copy.wait()


def loss_kernel(near, scale, place_ref, all_user_ref, all_target_ref, input_ref, *refs):
    sources = refs[:8]
    out_ref, weight_ref, candidate_ref, score_ref, user_ref, done, candidate_done, user_done = refs[8:]
    _, small, units, width = weight_ref.shape
    for i in (0, 3, 1, 2, 4, 7, 5, 6):
        pltpu.make_async_copy(sources[i].at[:, :units], weight_ref.at[i], done.at[i]).start()
    copies = [
        pltpu.make_async_copy(sources[i].at[:, units:], candidate_ref.at[i], candidate_done.at[i])
        for i in range(8)
    ]
    for copy in copies:
        copy.start()
    core, plane, home = place_ref[0], place_ref[1], (place_ref[4], place_ref[5])
    planes, rows, _ = input_ref.shape
    share = rows // CHUNKS
    targets, users = [], []
    for i in range(CHUNKS):
        start = (core * CHUNKS + i) * (planes * share) + plane * share
        start = pl.multiple_of(start, share)
        users.append(
            pltpu.make_async_copy(
                all_user_ref.at[pl.ds(start, share)],
                user_ref.at[i * share : (i + 1) * share],
                user_done.at[i],
            )
        )
        users[-1].start()
        values = jnp.broadcast_to(all_target_ref[pl.ds(start // LANES, 1)], (share, LANES))
        line = lax.broadcasted_iota(jnp.int32, (share, LANES), 0) + lax.rem(start, LANES)
        spots = lax.broadcasted_iota(jnp.int32, (share, LANES), 1)
        targets.append(jnp.sum(jnp.where(line == spots, values, 0), axis=1, keepdims=True))
    target = jnp.concatenate(targets, axis=0)
    contract = (((1,), (1,)), ((), ()))

    def inputs(which):
        at = pl.multiple_of(which * WIDE, WIDE)
        return jnp.concatenate([input_ref[z, :, pl.ds(at, WIDE)] for z in range(planes)], axis=1)

    def tower_step(n, gathered):
        owner, step = n // 2, n % 2
        spot = jnp.where(lax.rem(core + owner, 2) == 0, home[1], home[0])
        which = lax.rem(lax.rem(spot + step, 4) // 2 + core, 2)
        first, second = 4 * owner + step, 4 * owner + 3 - step
        for i in (first, second):
            pltpu.make_async_copy(weight_ref.at[i], weight_ref.at[i], done.at[i]).wait()
        a = weight_ref[first].reshape(small * units, width)
        b = weight_ref[second].reshape(small * units, width)
        pre = lax.dot_general(inputs(which), a, contract, preferred_element_type=jnp.float32)
        pre += lax.dot_general(inputs(1 - which), b, contract, preferred_element_type=jnp.float32)
        hidden = jnp.maximum(pre, 0.0).astype(jnp.bfloat16)
        tails = jnp.concatenate(
            [a[:, z * WIDE + LANES : (z + 1) * WIDE] for z in range(planes)], axis=1
        )
        return gathered + jnp.dot(hidden, tails, preferred_element_type=jnp.float32)

    gathered = lax.fori_loop(0, 4, tower_step, jnp.zeros((rows, planes * LANES), jnp.float32))
    lane = lax.broadcasted_iota(jnp.int32, (rows, LANES), 1)
    part = jnp.zeros((rows, LANES), jnp.float32)
    for z in range(planes):
        moved = pltpu.roll(gathered[:, z * LANES : (z + 1) * LANES], ((z - 5) * 16) % LANES, 1)
        part = jnp.where((lane >= z * 16) & (lane < (z + 1) * 16), moved, part)
    for copy in users:
        copy.wait()
    query = (part + user_ref[...].astype(jnp.float32)).astype(jnp.bfloat16)
    for copy in copies:
        copy.wait()
    lines = width // LANES
    count = lines * 8
    wide_lane = lax.broadcasted_iota(jnp.int32, (rows, count), 1)

    def score_step(number, state):
        picked, best = state
        place_in = number % 4
        far_offset = place_in ^ (place_in >> 1)
        from_core = lax.rem(core + number // 4, 2)
        for slot, near_offset in enumerate(near):
            rows_of = jnp.concatenate(
                [candidate_ref[number, slot, :, t * LANES : (t + 1) * LANES] for t in range(lines)],
                axis=0,
            )
            logits = (
                lax.dot_general(query, rows_of, contract, preferred_element_type=jnp.float32) * scale
            )
            outer = lax.rem(home[0] + jnp.where(from_core == 0, near_offset, far_offset), 4)
            inner = lax.rem(home[1] + jnp.where(from_core == 0, far_offset, near_offset), 4)
            base = (outer * 4 + inner) * (2 * count) + from_core * count
            picked += jnp.where(wide_lane == target - base, logits, 0.0)
            best = jnp.maximum(best, logits)
            score_ref[number * 4 + slot] = logits
        return picked, best

    picked, best = lax.fori_loop(
        0,
        8,
        score_step,
        (jnp.zeros((rows, count), jnp.float32), jnp.full((rows, count), -1e30, jnp.float32)),
    )
    picked = jnp.sum(picked, axis=1, keepdims=True)
    best = jnp.max(best, axis=1, keepdims=True)

    def total_step(i, total):
        return total + jnp.exp(score_ref[i] - best)

    total = lax.fori_loop(0, score_ref.shape[0], total_step, jnp.zeros((rows, count), jnp.float32))
    total = jnp.sum(total, axis=1, keepdims=True)
    loss = best + jnp.log(total) - picked
    row = lax.broadcasted_iota(jnp.int32, (rows, LANES), 0)
    spot = lax.rem(plane, LANES // share) * share
    for i in range(CHUNKS):
        mine = (row >= i * share) & (lane == row - i * share + spot)
        mine = mine & (row < (i + 1) * share)
        line = jnp.sum(jnp.where(mine, loss, 0.0), axis=0, keepdims=True)
        out_ref[:, i] = jnp.broadcast_to(line, (out_ref.shape[0], LANES))


def end_kernel(planes, lines_ref, out_ref):
    cores = lines_ref.shape[0] // planes
    groups = out_ref.shape[0] // (cores * CHUNKS)
    for c in range(cores):
        for i in range(CHUNKS):
            for g in range(groups):
                first = c * planes + g * (planes // groups)
                parts = [lines_ref[first + z, i : i + 1] for z in range(planes // groups)]
                at = (c * CHUNKS + i) * groups + g
                out_ref[at : at + 1] = functools.reduce(jnp.add, parts)


def over_planes(x):
    return lax.all_to_all(x, "dim", split_axis=0, concat_axis=0, tiled=True)


def over_all(x):
    return lax.all_to_all(x, ("field", "dim"), split_axis=0, concat_axis=0, tiled=True)


def program(
    features,
    cross_weight,
    cross_bias,
    tower_weight,
    tower_bias,
    query_weight,
    user_vec,
    candidates,
    positive,
):
    core = lax.axis_index("field")
    plane = lax.axis_index("dim")
    planes = lax.axis_size("dim")
    home = [lax.axis_index(axis) for axis in BATCH]
    field_local, entry_local, row_count = features.shape
    half_rows = row_count // 2
    chunk_rows = half_rows // CHUNKS
    share = chunk_rows // planes
    near_spot = jnp.where(core == 0, home[0], home[1])
    far_spot = jnp.where(core == 0, home[1], home[0])
    place = jnp.stack(
        [core, plane, far_spot // 2, 2 * near_spot + far_spot % 2, home[0], home[1]]
    ).astype(jnp.int32)

    def swap(x):
        return shift(x, "field", 1)

    half_count = field_local * entry_local
    count = 2 * half_count
    theirs, mine = pl.pallas_call(
        cut_kernel,
        out_shape=[jax.ShapeDtypeStruct((half_count, half_rows), jnp.bfloat16)] * 2,
        in_specs=[SMEM, HBM],
        out_specs=[VMEM] * 2,
        scratch_shapes=[pltpu.VMEM(features.shape, jnp.bfloat16), pltpu.SemaphoreType.DMA],
        compiler_params=grant(4),
    )(place, in_hbm(features))
    fetched = swap(theirs)
    weights = cross_weight.transpose(0, 1, 3, 2, 4)
    biases = cross_bias.transpose(1, 0, 2)

    other_weights = swap(weights)
    other_bias = swap(biases)

    piece = pl.pallas_call(
        pick_kernel,
        out_shape=jax.ShapeDtypeStruct((8 * planes, WIDE), jnp.bfloat16),
        in_specs=[SMEM, HBM, HBM, HBM],
        out_specs=VMEM,
        scratch_shapes=[
            pltpu.VMEM((field_local, 8, LANES), jnp.bfloat16),
            pltpu.VMEM((8, LANES), jnp.bfloat16),
            pltpu.SMEM(tower_bias.shape, jnp.float32),
            pltpu.SemaphoreType.DMA((3,)),
        ],
        compiler_params=grant(2),
    )(place, in_hbm(tower_bias), in_hbm(tower_weight.transpose(1, 0, 2)), in_hbm(query_weight))
    anchors = pl.pallas_call(
        join_kernel,
        out_shape=[
            jax.ShapeDtypeStruct((count + 8 * planes, chunk_rows), jnp.bfloat16),
            jax.ShapeDtypeStruct((count, chunk_rows), jnp.bfloat16),
        ],
        in_specs=[VMEM] * 3,
        out_specs=[VMEM] * 2,
        compiler_params=grant(4),
    )(mine, fetched, piece)
    rings = [ring_gather(anchors[0], "dim", True), ring_gather(anchors[1], "dim", False)]
    width = planes * WIDE
    stack = pl.pallas_call(
        functools.partial(stack_kernel, count),
        out_shape=jax.ShapeDtypeStruct((8 * planes + 8, width), jnp.bfloat16),
        in_specs=[SMEM] + [VMEM] * (1 + planes),
        out_specs=VMEM,
        compiler_params=grant(8),
    )(place, candidates, *[block for _, block in rings[0]])
    near_up = crosswise(stack, 1, False)
    near_down = crosswise(stack, -1, False)
    near_two = crosswise(stack, 2, False)
    near = (0, 3, 1, 2)
    block = pl.pallas_call(
        pile_kernel,
        out_shape=jax.ShapeDtypeStruct((4,) + stack.shape, stack.dtype),
        in_specs=[ANY] * 4,
        out_specs=ANY,
        scratch_shapes=[pltpu.SemaphoreType.DMA((4,))],
        compiler_params=grant(4),
    )(stack, near_up, near_down, near_two)
    far_down = crosswise(block, -1, True)
    far_up = crosswise(block, 1, True)
    far_two = crosswise(far_up, 1, True)
    own_arrays = [block, far_down, far_up, far_two]
    arrays = own_arrays + [swap(a) for a in own_arrays]
    for level in range(CROSS):
        matrix, bias = ordered_weight(level, place, weights, other_weights, biases, other_bias)
        results = []
        for i in range(CHUNKS):
            turn = i + 1 if level == CROSS - 1 else 0
            earlier = results[-1] if turn == 2 else []
            results.append(cross_layer(place, matrix, bias, anchors[i], rings[i], turn, earlier))
        if level < CROSS - 1:
            rings = [ring_gather(results[i][0], "dim", i % 2 == 0) for i in range(CHUNKS)]

    exchanged, partly, other_half = results[-1]
    exchanged = over_planes(exchanged)
    fetched = swap(other_half).reshape(field_local, entry_local, half_rows)
    crossed = pl.pallas_call(
        fill_kernel,
        out_shape=jax.ShapeDtypeStruct(partly.shape, partly.dtype),
        in_specs=[SMEM, VMEM, HBM],
        out_specs=HBM,
        input_output_aliases={2: 0},
        scratch_shapes=[pltpu.SemaphoreType.DMA],
        compiler_params=grant(2),
    )(place, fetched, partly)

    loss = pl.pallas_call(
        functools.partial(loss_kernel, near, 1.0 / math.sqrt(query_weight.shape[1])),
        out_shape=jax.ShapeDtypeStruct((2 * planes, CHUNKS, LANES), jnp.float32),
        in_specs=[SMEM, HBM, VMEM, VMEM] + [ANY] * len(arrays),
        out_specs=VMEM,
        scratch_shapes=[
            pltpu.VMEM((len(arrays), 4, 8 * planes, width), jnp.bfloat16),
            pltpu.VMEM((len(arrays), 4, 8, width), jnp.bfloat16),
            pltpu.VMEM((32, CHUNKS * share, width // 16), jnp.float32),
            pltpu.VMEM((CHUNKS * share, LANES), jnp.bfloat16),
            pltpu.SemaphoreType.DMA((len(arrays),)),
            pltpu.SemaphoreType.DMA((len(arrays),)),
            pltpu.SemaphoreType.DMA((CHUNKS,)),
        ],
        compiler_params=grant(20),
    )(place, user_vec, positive.reshape(-1, LANES), exchanged, *arrays)
    lines = over_all(loss)
    losses = pl.pallas_call(
        functools.partial(end_kernel, planes),
        out_shape=jax.ShapeDtypeStruct((row_count // LANES, LANES), jnp.float32),
        in_specs=[VMEM],
        out_specs=VMEM,
        compiler_params=grant(4),
    )(lines)
    return (crossed, losses.reshape(row_count))


def solution(mesh):
    torus = Mesh(
        mesh.devices.reshape(4, 4, mesh.shape["field"], mesh.shape["dim"]),
        ("batch_0", "batch_1", "field", "dim"),
    )
    in_specs = (
        P("field", "dim", BATCH),
        P(None, "field", "dim", None, None),
        P(None, "field", "dim"),
        P(("field", "dim"), None, None),
        P(("field", "dim")),
        P(("field", "dim"), None),
        P(BATCH, None),
        P(BATCH, None),
        P(BATCH),
    )
    out_specs = (P("field", "dim", BATCH), P(BATCH))
    return jax.shard_map(program, mesh=torus, in_specs=in_specs, out_specs=out_specs, check_vma=False)
```

```python
import functools
import math

import jax
import jax.numpy as jnp
from jax import lax
from jax.experimental import pallas as pl
from jax.experimental.pallas import tpu as pltpu
from jax.sharding import Mesh
from jax.sharding import PartitionSpec as P


CROSS = 2
BATCH = ("batch_0", "batch_1")
CHUNKS = 2
LANES = 128
WIDE = 256
SMEM = pl.BlockSpec(memory_space=pltpu.SMEM)
VMEM = pl.BlockSpec(memory_space=pltpu.VMEM)
ANY = pl.BlockSpec(memory_space=pl.ANY)
HBM = pl.BlockSpec(memory_space=pltpu.HBM)


def grant(mib):
    return pltpu.CompilerParams(vmem_limit_bytes=mib * 1024 * 1024)


def shift(x, axis, step):
    length = lax.axis_size(axis)
    return lax.ppermute(x, axis, [(i, (i + step) % length) for i in range(length)])


def ring_gather(block, axis, forward):
    length = lax.axis_size(axis)
    up = length // 2 if forward else length - 1 - length // 2
    down = length - 1 - up
    found = [(0, block)]
    rising = falling = block
    for step in range(1, max(up, down) + 1):
        if step <= up:
            rising = shift(rising, axis, 1)
            found.append((-step, rising))
        if step <= down:
            falling = shift(falling, axis, -1)
            found.append((step, falling))
    return found


def crosswise(x, step, far):
    outer, inner = (lax.axis_size(axis) for axis in BATCH)
    pairs = []
    for a in range(outer):
        for b in range(inner):
            for core in range(2):
                if (core == 0) != far:
                    target = ((a + step) % outer, b)
                else:
                    target = (a, (b + step) % inner)
                pairs.append((2 * (a * inner + b) + core, 2 * (target[0] * inner + target[1]) + core))
    return lax.ppermute(x, BATCH + ("field",), pairs)


def order_kernel(level, place_ref, own_ref, other_ref, bias_ref, other_bias_ref, out_ref, column_ref):
    core = place_ref[0]
    _, outer, fields, entries, lanes = own_ref.shape
    rows = outer * entries
    half = fields // 2

    def step(k, _):
        for part in range(2):
            group = 2 * k + part
            high = (group >= half).astype(jnp.int32)
            source = lax.rem(core + high, 2) * half + group - high * half
            span = slice(part * lanes, (part + 1) * lanes)
            out_ref[k, :rows, span] = own_ref[0, :, source].reshape(rows, lanes)
            out_ref[k, rows:, span] = other_ref[0, :, source].reshape(rows, lanes)
        return 0

    lax.fori_loop(0, fields // 2, step, 0)
    line = lax.broadcasted_iota(jnp.int32, (entries, entries), 0)
    lane = lax.broadcasted_iota(jnp.int32, (entries, entries), 1)
    for side, side_ref in enumerate((bias_ref, other_bias_ref)):
        for f in range(outer):
            values = side_ref[f, level : level + 1, :]
            turned = jnp.sum(jnp.where(line == lane, values, 0.0), axis=1, keepdims=True)
            at = side * rows + f * entries
            column_ref[at : at + entries, :] = jnp.broadcast_to(turned, (entries, LANES))


def ordered_weight(level, place, own, other, bias, other_bias):
    _, outer, fields, entries, lanes = own.shape
    rows = 2 * outer * entries
    part = pl.BlockSpec((1, outer, fields, entries, lanes), lambda i: (level, 0, 0, 0, 0))
    whole = pl.BlockSpec(bias.shape, lambda i: (0, 0, 0))
    out_shape = (
        jax.ShapeDtypeStruct((fields // 2, rows, 2 * lanes), own.dtype),
        jax.ShapeDtypeStruct((rows, LANES), jnp.float32),
    )
    return pl.pallas_call(
        functools.partial(order_kernel, level),
        grid=(1,),
        out_shape=out_shape,
        in_specs=[SMEM, part, part, whole, whole],
        out_specs=(
            pl.BlockSpec(out_shape[0].shape, lambda i: (0, 0, 0)),
            pl.BlockSpec(out_shape[1].shape, lambda i: (0, 0)),
        ),
        compiler_params=grant(14),
    )(place, own, other, bias, other_bias)


def layer_kernel(offsets, turn, place_ref, weight_ref, bias_ref, anchor_ref, *refs):
    length = len(offsets)
    blocks, refs = refs[:length], refs[length:]
    plane = place_ref[1]
    if turn:
        whole_ref, turned_ref, keep_ref, send_ref, done = refs[-5:]
        outs = refs[-8:-5]
    else:
        outs, whole_ref = refs[:1], refs[1]
    fields, _, entries, rows = whole_ref.shape
    count = fields * entries
    for offset, block_ref in zip(offsets, blocks):
        source = lax.rem(plane + offset + length, length)
        whole_ref[:, source] = block_ref[:count].reshape(fields, entries, rows)
    weight = jnp.concatenate([weight_ref[k] for k in range(weight_ref.shape[0])], axis=1)
    inputs = whole_ref[...].reshape(length * count, rows)
    product = jnp.dot(weight, inputs, preferred_element_type=jnp.float32) + bias_ref[:, :1]
    anchor = anchor_ref[:count].astype(jnp.float32)
    current = blocks[0][:count].astype(jnp.float32)
    result = (anchor * product + current).astype(jnp.bfloat16)
    if not turn:
        outs[0][...] = result
        return
    turn_ref, crossed_ref, other_ref = outs
    keep_ref[...] = result[: count // 2].reshape(keep_ref.shape)
    send_ref[...] = result[count // 2 :]
    half = other_ref.shape[1]
    first = (turn - 1) * rows
    start = pl.multiple_of(place_ref[0] * half + first, rows)
    copies = [
        pltpu.make_async_copy(keep_ref, crossed_ref.at[:, :, pl.ds(start, rows)], done.at[0]),
        pltpu.make_async_copy(send_ref, other_ref.at[:, pl.ds(first, rows)], done.at[1]),
    ]
    for copy in copies:
        copy.start()
    halves = result.reshape(2, count // 2, rows).astype(jnp.float32)
    spare = WIDE - count // 2
    share = rows // length
    line = lax.broadcasted_iota(jnp.int32, (spare, rows), 0)
    ones = jnp.where((line >= 16) & (line < 19), 1.0, 0.0)
    for h in range(2):
        turned = jnp.concatenate([halves[h], ones], axis=0).T.astype(jnp.bfloat16)
        turned_ref[h] = turned.reshape(length, share, WIDE)
        span = slice(h * WIDE, (h + 1) * WIDE)
        target = turn_ref.at[:, pl.ds((turn - 1) * share, share), span]
        copies.append(pltpu.make_async_copy(turned_ref.at[h], target, done.at[2 + h]))
        copies[-1].start()
    for copy in copies:
        copy.wait()


def cross_layer(place, matrix, bias, anchor, found, turn, earlier):
    offsets = tuple(offset for offset, _ in found)
    blocks = [block for _, block in found]
    count, rows = matrix.shape[1], anchor.shape[1]
    planes = len(blocks)
    out_shape = [jax.ShapeDtypeStruct((count, rows), jnp.bfloat16)]
    scratch = [pltpu.VMEM((count // 16, planes, 16, rows), jnp.bfloat16)]
    if turn:
        fields = count // 32
        out_shape = [
            pltpu.HBM((planes, CHUNKS * rows // planes, 2 * WIDE), jnp.bfloat16),
            pltpu.HBM((fields, 16, 2 * CHUNKS * rows), jnp.bfloat16),
            pltpu.HBM((count // 2, CHUNKS * rows), jnp.bfloat16),
        ]
        scratch += [
            pltpu.VMEM((2, planes, rows // planes, WIDE), jnp.bfloat16),
            pltpu.VMEM((fields, 16, rows), jnp.bfloat16),
            pltpu.VMEM((count // 2, rows), jnp.bfloat16),
            pltpu.SemaphoreType.DMA((4,)),
        ]
    base = 4 + planes
    return pl.pallas_call(
        functools.partial(layer_kernel, offsets, turn),
        out_shape=out_shape,
        in_specs=[SMEM] + [VMEM] * (3 + planes) + [HBM] * len(earlier),
        out_specs=[HBM] * 3 if turn else [VMEM],
        input_output_aliases={base + i: i for i in range(len(earlier))},
        scratch_shapes=scratch,
        compiler_params=grant(14),
    )(place, matrix, bias, anchor, *blocks, *earlier)


def in_hbm(x):
    return pltpu.with_memory_space_constraint(x, pltpu.HBM)


def fill_kernel(place_ref, fetched_ref, given_ref, crossed_ref, done):
    half = fetched_ref.shape[2]
    start = pl.multiple_of((1 - place_ref[0]) * half, half)
    copy = pltpu.make_async_copy(fetched_ref, crossed_ref.at[:, :, pl.ds(start, half)], done)
    copy.start()
    copy.wait()


def cut_kernel(place_ref, feature_ref, theirs_ref, mine_ref, whole_ref, done):
    copy = pltpu.make_async_copy(feature_ref, whole_ref, done)
    copy.start()
    copy.wait()
    count, half = theirs_ref.shape
    for side, out_ref in enumerate((mine_ref, theirs_ref)):
        start = pl.multiple_of(jnp.abs(side - place_ref[0]) * half, half)
        out_ref[...] = whole_ref[:, :, pl.ds(start, half)].reshape(count, half)


def pick_kernel(
    place_ref, all_bias_ref, tower_ref, query_ref, piece_ref, part_ref, row_ref, bias_ref, done
):
    high, group = place_ref[2], place_ref[3]
    half, count, _ = part_ref.shape
    entries = 16
    planes = LANES // entries
    start = pl.multiple_of(group * count, count)
    copies = [
        pltpu.make_async_copy(
            tower_ref.at[pl.ds(high * half, half), pl.ds(start, count)], part_ref, done.at[0]
        ),
        pltpu.make_async_copy(query_ref.at[pl.ds(start, count)], row_ref, done.at[1]),
        pltpu.make_async_copy(all_bias_ref, bias_ref, done.at[2]),
    ]
    for copy in copies:
        copy.start()
    for copy in copies:
        copy.wait()
    lane = lax.broadcasted_iota(jnp.int32, (count, LANES), 1)
    line = lax.broadcasted_iota(jnp.int32, (count, LANES), 0)
    bias = jnp.zeros((count, LANES), jnp.float32)
    for u in range(count):
        bias = jnp.where(line == u, bias_ref[start + u], bias)
    sources = [part_ref[f].astype(jnp.float32) for f in range(half)]
    query = row_ref[...].astype(jnp.float32)
    first = bias.astype(jnp.bfloat16).astype(jnp.float32)
    second = (bias - first).astype(jnp.bfloat16).astype(jnp.float32)
    third = bias - first - second
    bias_lanes = jnp.where(
        lane == 96, first, jnp.where(lane == 97, second, jnp.where(lane == 98, third, 0.0))
    )
    bias_lanes = jnp.where(high == 0, bias_lanes, 0.0)
    for plane in range(planes):
        for tile in range(2):
            kept = bias_lanes if (tile == 1 and plane == 0) else jnp.zeros((count, LANES), jnp.float32)
            inside = [(f % 8, sources[f]) for f in range(half) if f // 8 == tile]
            if tile == 1:
                inside.append((5, query))
            for slot, source in inside:
                moved = pltpu.roll(source, ((slot - plane) * entries) % LANES, 1)
                kept = jnp.where((lane >= slot * entries) & (lane < (slot + 1) * entries), moved, kept)
            span = slice(tile * LANES, (tile + 1) * LANES)
            piece_ref[plane * count : (plane + 1) * count, span] = kept.astype(jnp.bfloat16)


def join_kernel(mine_ref, other_ref, piece_ref, first_ref, second_ref):
    half_count, half_rows = other_ref.shape
    rows = half_rows // CHUNKS
    for i, block_ref in enumerate((first_ref, second_ref)):
        span = slice(i * rows, (i + 1) * rows)
        block_ref[:half_count] = mine_ref[:, span]
        block_ref[half_count : 2 * half_count] = other_ref[:, span]
    first_ref[2 * half_count :] = piece_ref[...]


def stack_kernel(first_row, place_ref, candidate_ref, *refs):
    blocks, out_ref = refs[:-1], refs[-1]
    planes = len(blocks)
    for source, block_ref in enumerate(blocks):
        for z in range(planes):
            at = first_row + z * 8
            out_ref[source * 8 : source * 8 + 8, z * WIDE : (z + 1) * WIDE] = block_ref[at : at + 8]
    units = planes * 8
    lines = out_ref.shape[1] // LANES
    for t in range(lines):
        at = pl.multiple_of(place_ref[0] * (8 * lines) + t * 8, 8)
        out_ref[units:, t * LANES : (t + 1) * LANES] = candidate_ref[pl.ds(at, 8)]


def pile_kernel(*refs):
    parts, out_ref, done = refs[:-2], refs[-2], refs[-1]
    copies = [
        pltpu.make_async_copy(part_ref, out_ref.at[i], done.at[i]) for i, part_ref in enumerate(parts)
    ]
    for copy in copies:
        copy.start()
    for copy in copies:
        copy.wait()


def loss_kernel(near, scale, place_ref, all_user_ref, all_target_ref, input_ref, *refs):
    sources = refs[:8]
    out_ref, weight_ref, candidate_ref, score_ref, user_ref, done, candidate_done, user_done = refs[8:]
    _, small, units, width = weight_ref.shape
    for i in (0, 3, 1, 2, 4, 7, 5, 6):
        pltpu.make_async_copy(sources[i].at[:, :units], weight_ref.at[i], done.at[i]).start()
    copies = [
        pltpu.make_async_copy(sources[i].at[:, units:], candidate_ref.at[i], candidate_done.at[i])
        for i in range(8)
    ]
    for copy in copies:
        copy.start()
    core, plane, home = place_ref[0], place_ref[1], (place_ref[4], place_ref[5])
    planes, rows, _ = input_ref.shape
    share = rows // CHUNKS
    targets, users = [], []
    for i in range(CHUNKS):
        start = (core * CHUNKS + i) * (planes * share) + plane * share
        start = pl.multiple_of(start, share)
        users.append(
            pltpu.make_async_copy(
                all_user_ref.at[pl.ds(start, share)],
                user_ref.at[i * share : (i + 1) * share],
                user_done.at[i],
            )
        )
        users[-1].start()
        values = jnp.broadcast_to(all_target_ref[pl.ds(start // LANES, 1)], (share, LANES))
        line = lax.broadcasted_iota(jnp.int32, (share, LANES), 0) + lax.rem(start, LANES)
        spots = lax.broadcasted_iota(jnp.int32, (share, LANES), 1)
        targets.append(jnp.sum(jnp.where(line == spots, values, 0), axis=1, keepdims=True))
    target = jnp.concatenate(targets, axis=0)
    contract = (((1,), (1,)), ((), ()))

    def inputs(which):
        at = pl.multiple_of(which * WIDE, WIDE)
        return jnp.concatenate([input_ref[z, :, pl.ds(at, WIDE)] for z in range(planes)], axis=1)

    def tower_step(n, gathered):
        owner, step = n // 2, n % 2
        spot = jnp.where(lax.rem(core + owner, 2) == 0, home[1], home[0])
        which = lax.rem(lax.rem(spot + step, 4) // 2 + core, 2)
        first, second = 4 * owner + step, 4 * owner + 3 - step
        for i in (first, second):
            pltpu.make_async_copy(weight_ref.at[i], weight_ref.at[i], done.at[i]).wait()
        a = weight_ref[first].reshape(small * units, width)
        b = weight_ref[second].reshape(small * units, width)
        pre = lax.dot_general(inputs(which), a, contract, preferred_element_type=jnp.float32)
        pre += lax.dot_general(inputs(1 - which), b, contract, preferred_element_type=jnp.float32)
        hidden = jnp.maximum(pre, 0.0).astype(jnp.bfloat16)
        tails = jnp.concatenate(
            [a[:, z * WIDE + LANES : (z + 1) * WIDE] for z in range(planes)], axis=1
        )
        return gathered + jnp.dot(hidden, tails, preferred_element_type=jnp.float32)

    gathered = lax.fori_loop(0, 4, tower_step, jnp.zeros((rows, planes * LANES), jnp.float32))
    lane = lax.broadcasted_iota(jnp.int32, (rows, LANES), 1)
    part = jnp.zeros((rows, LANES), jnp.float32)
    for z in range(planes):
        moved = pltpu.roll(gathered[:, z * LANES : (z + 1) * LANES], ((z - 5) * 16) % LANES, 1)
        part = jnp.where((lane >= z * 16) & (lane < (z + 1) * 16), moved, part)
    for copy in users:
        copy.wait()
    query = (part + user_ref[...].astype(jnp.float32)).astype(jnp.bfloat16)
    for copy in copies:
        copy.wait()
    lines = width // LANES
    count = lines * 8
    wide_lane = lax.broadcasted_iota(jnp.int32, (rows, count), 1)

    def score_step(number, state):
        picked, best = state
        place_in = number % 4
        far_offset = place_in ^ (place_in >> 1)
        from_core = lax.rem(core + number // 4, 2)
        rows_of = jnp.concatenate(
            [
                candidate_ref[number, slot, :, t * LANES : (t + 1) * LANES]
                for slot in range(len(near))
                for t in range(lines)
            ],
            axis=0,
        )
        scores = lax.dot_general(query, rows_of, contract, preferred_element_type=jnp.float32)
        for slot, near_offset in enumerate(near):
            logits = scores[:, slot * count : (slot + 1) * count] * scale
            outer = lax.rem(home[0] + jnp.where(from_core == 0, near_offset, far_offset), 4)
            inner = lax.rem(home[1] + jnp.where(from_core == 0, far_offset, near_offset), 4)
            base = (outer * 4 + inner) * (2 * count) + from_core * count
            picked += jnp.where(wide_lane == target - base, logits, 0.0)
            best = jnp.maximum(best, logits)
            score_ref[number * 4 + slot] = logits
        return picked, best

    picked, best = lax.fori_loop(
        0,
        8,
        score_step,
        (jnp.zeros((rows, count), jnp.float32), jnp.full((rows, count), -1e30, jnp.float32)),
    )
    picked = jnp.sum(picked, axis=1, keepdims=True)
    best = jnp.max(best, axis=1, keepdims=True)

    def total_step(i, total):
        return total + jnp.exp(score_ref[i] - best)

    total = lax.fori_loop(0, score_ref.shape[0], total_step, jnp.zeros((rows, count), jnp.float32))
    total = jnp.sum(total, axis=1, keepdims=True)
    loss = best + jnp.log(total) - picked
    row = lax.broadcasted_iota(jnp.int32, (rows, LANES), 0)
    spot = lax.rem(plane, LANES // share) * share
    for i in range(CHUNKS):
        mine = (row >= i * share) & (lane == row - i * share + spot)
        mine = mine & (row < (i + 1) * share)
        line = jnp.sum(jnp.where(mine, loss, 0.0), axis=0, keepdims=True)
        out_ref[:, i] = jnp.broadcast_to(line, (out_ref.shape[0], LANES))


def end_kernel(planes, lines_ref, out_ref):
    cores = lines_ref.shape[0] // planes
    groups = out_ref.shape[0] // (cores * CHUNKS)
    for c in range(cores):
        for i in range(CHUNKS):
            for g in range(groups):
                first = c * planes + g * (planes // groups)
                parts = [lines_ref[first + z, i : i + 1] for z in range(planes // groups)]
                at = (c * CHUNKS + i) * groups + g
                out_ref[at : at + 1] = functools.reduce(jnp.add, parts)


def over_planes(x):
    return lax.all_to_all(x, "dim", split_axis=0, concat_axis=0, tiled=True)


def over_all(x):
    return lax.all_to_all(x, ("field", "dim"), split_axis=0, concat_axis=0, tiled=True)


def program(
    features,
    cross_weight,
    cross_bias,
    tower_weight,
    tower_bias,
    query_weight,
    user_vec,
    candidates,
    positive,
):
    core = lax.axis_index("field")
    plane = lax.axis_index("dim")
    planes = lax.axis_size("dim")
    home = [lax.axis_index(axis) for axis in BATCH]
    field_local, entry_local, row_count = features.shape
    half_rows = row_count // 2
    chunk_rows = half_rows // CHUNKS
    share = chunk_rows // planes
    near_spot = jnp.where(core == 0, home[0], home[1])
    far_spot = jnp.where(core == 0, home[1], home[0])
    place = jnp.stack(
        [core, plane, far_spot // 2, 2 * near_spot + far_spot % 2, home[0], home[1]]
    ).astype(jnp.int32)

    def swap(x):
        return shift(x, "field", 1)

    half_count = field_local * entry_local
    count = 2 * half_count
    theirs, mine = pl.pallas_call(
        cut_kernel,
        out_shape=[jax.ShapeDtypeStruct((half_count, half_rows), jnp.bfloat16)] * 2,
        in_specs=[SMEM, HBM],
        out_specs=[VMEM] * 2,
        scratch_shapes=[pltpu.VMEM(features.shape, jnp.bfloat16), pltpu.SemaphoreType.DMA],
        compiler_params=grant(4),
    )(place, in_hbm(features))
    fetched = swap(theirs)
    weights = cross_weight.transpose(0, 1, 3, 2, 4)
    biases = cross_bias.transpose(1, 0, 2)

    other_weights = swap(weights)
    other_bias = swap(biases)

    piece = pl.pallas_call(
        pick_kernel,
        out_shape=jax.ShapeDtypeStruct((8 * planes, WIDE), jnp.bfloat16),
        in_specs=[SMEM, HBM, HBM, HBM],
        out_specs=VMEM,
        scratch_shapes=[
            pltpu.VMEM((field_local, 8, LANES), jnp.bfloat16),
            pltpu.VMEM((8, LANES), jnp.bfloat16),
            pltpu.SMEM(tower_bias.shape, jnp.float32),
            pltpu.SemaphoreType.DMA((3,)),
        ],
        compiler_params=grant(2),
    )(place, in_hbm(tower_bias), in_hbm(tower_weight.transpose(1, 0, 2)), in_hbm(query_weight))
    anchors = pl.pallas_call(
        join_kernel,
        out_shape=[
            jax.ShapeDtypeStruct((count + 8 * planes, chunk_rows), jnp.bfloat16),
            jax.ShapeDtypeStruct((count, chunk_rows), jnp.bfloat16),
        ],
        in_specs=[VMEM] * 3,
        out_specs=[VMEM] * 2,
        compiler_params=grant(4),
    )(mine, fetched, piece)
    rings = [ring_gather(anchors[0], "dim", True), ring_gather(anchors[1], "dim", False)]
    width = planes * WIDE
    stack = pl.pallas_call(
        functools.partial(stack_kernel, count),
        out_shape=jax.ShapeDtypeStruct((8 * planes + 8, width), jnp.bfloat16),
        in_specs=[SMEM] + [VMEM] * (1 + planes),
        out_specs=VMEM,
        compiler_params=grant(8),
    )(place, candidates, *[block for _, block in rings[0]])
    near_up = crosswise(stack, 1, False)
    near_down = crosswise(stack, -1, False)
    near_two = crosswise(stack, 2, False)
    near = (0, 3, 1, 2)
    block = pl.pallas_call(
        pile_kernel,
        out_shape=jax.ShapeDtypeStruct((4,) + stack.shape, stack.dtype),
        in_specs=[ANY] * 4,
        out_specs=ANY,
        scratch_shapes=[pltpu.SemaphoreType.DMA((4,))],
        compiler_params=grant(4),
    )(stack, near_up, near_down, near_two)
    far_down = crosswise(block, -1, True)
    far_up = crosswise(block, 1, True)
    far_two = crosswise(far_up, 1, True)
    own_arrays = [block, far_down, far_up, far_two]
    arrays = own_arrays + [swap(a) for a in own_arrays]
    for level in range(CROSS):
        matrix, bias = ordered_weight(level, place, weights, other_weights, biases, other_bias)
        results = []
        for i in range(CHUNKS):
            turn = i + 1 if level == CROSS - 1 else 0
            earlier = results[-1] if turn == 2 else []
            results.append(cross_layer(place, matrix, bias, anchors[i], rings[i], turn, earlier))
        if level < CROSS - 1:
            rings = [ring_gather(results[i][0], "dim", i % 2 == 0) for i in range(CHUNKS)]

    exchanged, partly, other_half = results[-1]
    exchanged = over_planes(exchanged)
    fetched = swap(other_half).reshape(field_local, entry_local, half_rows)
    crossed = pl.pallas_call(
        fill_kernel,
        out_shape=jax.ShapeDtypeStruct(partly.shape, partly.dtype),
        in_specs=[SMEM, VMEM, HBM],
        out_specs=HBM,
        input_output_aliases={2: 0},
        scratch_shapes=[pltpu.SemaphoreType.DMA],
        compiler_params=grant(2),
    )(place, fetched, partly)

    loss = pl.pallas_call(
        functools.partial(loss_kernel, near, 1.0 / math.sqrt(query_weight.shape[1])),
        out_shape=jax.ShapeDtypeStruct((2 * planes, CHUNKS, LANES), jnp.float32),
        in_specs=[SMEM, HBM, VMEM, VMEM] + [ANY] * len(arrays),
        out_specs=VMEM,
        scratch_shapes=[
            pltpu.VMEM((len(arrays), 4, 8 * planes, width), jnp.bfloat16),
            pltpu.VMEM((len(arrays), 4, 8, width), jnp.bfloat16),
            pltpu.VMEM((32, CHUNKS * share, width // 16), jnp.float32),
            pltpu.VMEM((CHUNKS * share, LANES), jnp.bfloat16),
            pltpu.SemaphoreType.DMA((len(arrays),)),
            pltpu.SemaphoreType.DMA((len(arrays),)),
            pltpu.SemaphoreType.DMA((CHUNKS,)),
        ],
        compiler_params=grant(20),
    )(place, user_vec, positive.reshape(-1, LANES), exchanged, *arrays)
    lines = over_all(loss)
    losses = pl.pallas_call(
        functools.partial(end_kernel, planes),
        out_shape=jax.ShapeDtypeStruct((row_count // LANES, LANES), jnp.float32),
        in_specs=[VMEM],
        out_specs=VMEM,
        compiler_params=grant(4),
    )(lines)
    return (crossed, losses.reshape(row_count))


def solution(mesh):
    torus = Mesh(
        mesh.devices.reshape(4, 4, mesh.shape["field"], mesh.shape["dim"]),
        ("batch_0", "batch_1", "field", "dim"),
    )
    in_specs = (
        P("field", "dim", BATCH),
        P(None, "field", "dim", None, None),
        P(None, "field", "dim"),
        P(("field", "dim"), None, None),
        P(("field", "dim")),
        P(("field", "dim"), None),
        P(BATCH, None),
        P(BATCH, None),
        P(BATCH),
    )
    out_specs = (P("field", "dim", BATCH), P(BATCH))
    return jax.shard_map(program, mesh=torus, in_specs=in_specs, out_specs=out_specs, check_vma=False)
```
